256 devices in a mesh: dp: 32 (over z, x), mp: 4 (over y), mc: 2 (over core).
Axes of the slice: x: 4, y: 4, z: 8, core: 2. Of those that a mesh axis runs over, the one named last changes fastest.
Arguments:
- features: bfloat16 [12608, 768], P('dp'), may hold values from -6 to 6
- out_cotangent: bfloat16 [2, 12608, 768], P('mc', 'dp'), may hold values from -6 to 6
- mean_up: float32 [768, 3072], P('dp', 'mp'), may hold values from -0.21875 to 0.21875
- precision_up: float32 [768, 3072], P('dp', 'mp'), may hold values from 4 to 64
- noise_up: float32 [2, 768, 3072], P('mc', 'dp', 'mp'), may hold values from -6 to 6
- mean_down: float32 [768, 3072], P('dp', 'mp'), may hold values from -0.109375 to 0.109375
- precision_down: float32 [768, 3072], P('dp', 'mp'), may hold values from 4 to 64
- noise_down: float32 [2, 768, 3072], P('mc', 'dp', 'mp'), may hold values from -6 to 6
Outputs:
- mean_new_up: float32 [768, 3072], P('dp', 'mp')
- precision_new_up: float32 [768, 3072], P('dp', 'mp')
- mean_new_down: float32 [768, 3072], P('dp', 'mp')
- precision_new_down: float32 [768, 3072], P('dp', 'mp')
- input_grad: bfloat16 [2, 12608, 768], P('mc', 'dp', 'mp')
The draws below stay inside these ranges and needn't reach their ends.
All inputs are finite; a program needn't handle non-finite values.
Results may differ from the reference program's by a relative error of at most 0.0015.
The reference program's roundings to bfloat16 on the way (of `hidden` and `preact_grad`) count: a program that leaves them out, or rounds other values in their place, can miss the bound.
Values may be sent and summed in bfloat16 or wider, within the bound.
No kernel may reach another device: no remote copies, remote signals or barrier semaphores. Data moves between devices by JAX's collectives and lax.ppermute only.
A program may use at most 64 MiB of HBM per device.

```python
import math
import jax
import jax.numpy as jnp
from jax import lax

D = 768
FF = 3072
PATCHES = 197
MC = 2
IMAGES = 64
TOKENS = 12608


def raised(result, key, source, target, blocks, factor):
    def block_of(axis_at):
        return (jnp.arange(result.shape[axis_at]) // (result.shape[axis_at] // blocks)).reshape((-1,) + (1,) * (result.ndim - 1 - axis_at))

    one_side = jax.random.permutation(key, blocks)[block_of(target)]
    other_side = (block_of(target) + blocks // 2) % blocks
    return jnp.where((block_of(source) == one_side) | (block_of(source) == other_side), factor * result, result)


def block_scale(rng, extent, cuts, low, largest):
    level, own = 1.0, jax.random.fold_in(rng, 6)
    for position, shards_of in cuts:
        steps = jnp.exp(jax.random.uniform(jax.random.fold_in(own, position), (shards_of,), jnp.float32, low / len(cuts), largest / len(cuts)))
        level = level * jnp.repeat(steps, extent[position] // shards_of).reshape([-1 if axis == position else 1 for axis in range(len(extent))])
    return level


def scatter_about(stream_key, dims, width, limit, split=(), held_as=jnp.bfloat16):
    drawn = width * jax.random.normal(stream_key, dims, jnp.float32)
    if split:
        drawn = drawn * block_scale(stream_key, dims, split, -0.22, 0.18)
    return jnp.clip(drawn, -limit, limit).astype(held_as)


def bell_draw_with(own_key, extent, scale, bound, split, heavy, dtype=jnp.bfloat16):
    values = scale * jax.random.normal(own_key, extent, jnp.float32)
    if split:
        values = values * block_scale(own_key, extent, split, -0.22, 0.18)
    return jnp.clip(raised(values, jax.random.fold_in(own_key, 3), *heavy), -bound, bound).astype(dtype)


def setup_inputs(seed: int = 0) -> dict:
    key_list = jax.random.split(jax.random.key(seed), 9)
    return {
        "features": bell_draw_with(key_list[0], (TOKENS, D), 1.0, 6.0, ((0, 32),), (0, 1, 32, 2.75)),
        "out_cotangent": bell_draw_with(key_list[1], (MC, TOKENS, D), 1.0, 6.0, ((0, 2), (1, 32)), (1, 2, 32, 2.75)),
        "mean_up": scatter_about(key_list[2], (D, FF), D ** -0.5, 0.21875, ((0, 32), (1, 4)), jnp.float32),
        "precision_up": jnp.clip(jnp.exp(math.log(64.0) - 2.7725887 * jax.random.uniform(key_list[3], (D, FF), jnp.float32) ** block_scale(key_list[3], (D, FF), ((0, 32), (1, 4)), -0.2, 0.2)), 4.0, 64.0),
        "noise_up": scatter_about(key_list[4], (MC, D, FF), 1.0, 6.0, ((0, 2), (1, 32), (2, 4)), jnp.float32),
        "mean_down": scatter_about(key_list[5], (D, FF), FF ** -0.5, 0.109375, ((0, 32), (1, 4)), jnp.float32),
        "precision_down": jnp.clip(jnp.exp(math.log(64.0) - 2.7725887 * jax.random.uniform(key_list[6], (D, FF), jnp.float32) ** block_scale(key_list[6], (D, FF), ((0, 32), (1, 4)), -0.2, 0.2)), 4.0, 64.0),
        "noise_down": scatter_about(key_list[7], (MC, D, FF), 1.0, 6.0, ((0, 2), (1, 32), (2, 4)), jnp.float32),
    }


reciprocal_root = 0.7071067811865476
normal_peak = 0.3989422804014327
tempering = 100.0
damping = 4.0
average_rate = 0.25
step_rate = 0.05
clip_level = 0.01

def gelu_parts(preact):
    cumulative = 0.5 * (1.0 + lax.erf(preact * reciprocal_root))
    density = normal_peak * jnp.exp(-0.5 * preact * preact)
    return (preact * cumulative, cumulative + preact * density)

def sample_weights(center, precision, noise_draw):
    spread = 1.0 / jnp.sqrt(tempering * (precision + damping))
    return (center + spread * noise_draw).astype(jnp.bfloat16)

def contract_rows(left, right):
    return lax.dot_general(left, right, (((0,), (0,)), ((), ())), preferred_element_type=jnp.float32)

def contract_cols(left, right):
    return lax.dot_general(left, right, (((1,), (1,)), ((), ())), preferred_element_type=jnp.float32)

def reference(features, out_cotangent, mean_up, precision_up, noise_up, mean_down, precision_down, noise_down):
    images = features.shape[0] // PATCHES
    pictures = features.reshape(images, PATCHES, D)
    empty_sum = jnp.zeros((D, FF), jnp.float32)
    running = (empty_sum, empty_sum, empty_sum, empty_sum)
    gradients = []
    for sample_index in range(MC):
        w_up = sample_weights(mean_up, precision_up, noise_up[sample_index])
        w_down = sample_weights(mean_down, precision_down, noise_down[sample_index])
        cotangent = out_cotangent[sample_index].reshape(images, PATCHES, D)

        def per_image(totals, image_pair):
            image_rows, cotangent_rows = image_pair
            preact = jnp.dot(image_rows, w_up, preferred_element_type=jnp.float32)
            gelu_value, gelu_slope = gelu_parts(preact)
            hidden = gelu_value.astype(jnp.bfloat16)
            hidden_grad = jnp.dot(cotangent_rows, w_down, preferred_element_type=jnp.float32)
            preact_grad = (hidden_grad * gelu_slope).astype(jnp.bfloat16)
            input_rows = contract_cols(preact_grad, w_up).astype(jnp.bfloat16)
            grad_up = contract_rows(image_rows, preact_grad)
            grad_down = contract_rows(cotangent_rows, hidden)
            updated = (totals[0] + grad_up, totals[1] + grad_up * grad_up, totals[2] + grad_down, totals[3] + grad_down * grad_down)
            return (updated, input_rows)
        running, input_rows = lax.scan(per_image, running, (pictures, cotangent))
        gradients.append(input_rows.reshape(images * PATCHES, D))
    input_grad = jnp.stack(gradients)
    grad_up = running[0] / MC
    square_up = running[1] / (MC * IMAGES)
    grad_down = running[2] / MC
    square_down = running[3] / (MC * IMAGES)
    precision_new_up = (1.0 - average_rate) * precision_up + average_rate * square_up
    precision_new_down = (1.0 - average_rate) * precision_down + average_rate * square_down
    raw_up = grad_up / (precision_new_up + damping)
    raw_down = grad_down / (precision_new_down + damping)
    global_sum = jnp.sum(raw_up * raw_up) + jnp.sum(raw_down * raw_down)
    root_mean = jnp.sqrt(global_sum / (2 * D * FF))
    factor = 1.0 / jnp.maximum(clip_level, root_mean)
    mean_new_up = mean_up - step_rate * factor * raw_up
    mean_new_down = mean_down - step_rate * factor * raw_down
    return (mean_new_up, precision_new_up, mean_new_down, precision_new_down, input_grad)
```

```python
import jax
import jax.numpy as jnp
from jax import lax
from jax.sharding import Mesh
from jax.sharding import PartitionSpec as P

D = 768
FF = 3072
PATCHES = 197
PAD = 208
DP = ("z", "x")
ZXY = ("z", "x", "mp")

reciprocal_root = 0.7071067811865476
normal_peak = 0.3989422804014327
tempering = 100.0
damping = 4.0
average_rate = 0.25
step_rate = 0.05
clip_level = 0.01


def gelu_parts(preact):
    cumulative = 0.5 * (1.0 + lax.erf(preact * reciprocal_root))
    density = normal_peak * jnp.exp(-0.5 * preact * preact)
    return (preact * cumulative, cumulative + preact * density)


def sample_weights(center, precision, noise_draw):
    spread = 1.0 / jnp.sqrt(tempering * (precision + damping))
    return (center + spread * noise_draw).astype(jnp.bfloat16)


def shift(value, axis, k):
    n = lax.axis_size(axis)
    return lax.ppermute(value, axis, [(i, (i + k) % n) for i in range(n)])


def swap_cores(value):
    return lax.ppermute(value, "mc", [(0, 1), (1, 0)])


def padded(rows, core):
    images = jnp.pad(rows.reshape(2, PATCHES, D), ((0, 0), (0, PAD - PATCHES), (0, 0)))
    return jnp.where(core == 0, images, images[::-1])


def shards(
    features, out_cotangent, mean_up, precision_up, noise_up, mean_down, precision_down, noise_down
):
    core = lax.axis_index("mc")
    nz, nx = lax.axis_size("z"), lax.axis_size("x")
    rows, cols = mean_up.shape
    wide = cols // nx

    up = sample_weights(mean_up, precision_up, noise_up[0]).reshape(rows, nx, wide)
    down = sample_weights(mean_down, precision_down, noise_down[0]).reshape(rows, nx, wide)
    out = jnp.moveaxis(jnp.concatenate([up, down], axis=2), 1, 0)
    out = jnp.broadcast_to(out[None], (nz, nx, rows, 2 * wide)).reshape(nz * nx, rows, 2 * wide)
    weights = lax.all_to_all(out, DP, 0, 0, tiled=True).reshape(D, 2 * wide)
    w_up, w_down = weights[:, :wide], weights[:, wide:]

    own_f = padded(features, core)
    own_c = padded(out_cotangent[0], core).reshape(2 * PAD, D)
    sent = jnp.concatenate([own_f[0], own_c], axis=0)
    half = sent.shape[0] // 2
    right = shift(sent, "x", 1)
    left = shift(sent, "x", -1)
    far = jnp.concatenate([shift(right[:half], "x", 1), shift(left[half:], "x", -1)], axis=0)
    arrived = [right, left, far]
    mine = jnp.stack([a[:PAD] for a in arrived])
    other = swap_cores(mine)
    f_all = jnp.concatenate(
        [own_f.reshape(1, 2, PAD, D), jnp.stack([mine, other], axis=1)], axis=0
    ).reshape(8 * PAD, D)
    c_all = jnp.concatenate([own_c] + [a[PAD:] for a in arrived], axis=0)

    preact = jnp.dot(f_all, w_up, preferred_element_type=jnp.float32)
    gelu_value, gelu_slope = gelu_parts(preact)
    hidden = gelu_value.astype(jnp.bfloat16)
    hidden_grad = jnp.dot(c_all, w_down, preferred_element_type=jnp.float32)
    preact_grad = (hidden_grad * gelu_slope).astype(jnp.bfloat16)

    def sums(left, right):
        each = jnp.einsum(
            "ird,irf->idf",
            left.reshape(8, PAD, D),
            right.reshape(8, PAD, wide),
            preferred_element_type=jnp.float32,
        )
        return jnp.stack([jnp.sum(each, axis=0), jnp.sum(each * each, axis=0)])

    both = jnp.stack([sums(f_all, preact_grad), sums(c_all, hidden)])
    traded = lax.all_to_all(both, "mc", 0, 0, tiled=True)
    half_sum = (traded[0] + traded[1]).reshape(2, nz * nx, rows, wide)
    sent_sum = jnp.moveaxis(half_sum, 0, 1).reshape(nz * nx, 2 * rows, wide)
    got = lax.all_to_all(sent_sum, DP, 0, 0, tiled=True).reshape(nz, nx, 2, rows, wide)
    total = jnp.moveaxis(jnp.sum(got, axis=0), 0, 2).reshape(2, rows, cols)
    totals = lax.all_gather(total, "mc", axis=0)

    pg = preact_grad.reshape(4, 2 * PAD, wide)
    back = [(pg[0], w_up)] + [
        (shift(pg[i], "x", -k), shift(w_up, "x", -k)) for i, k in ((1, 1), (2, -1), (3, 2))
    ]
    partial_value = sum(
        lax.dot_general(a, b, (((1,), (1,)), ((), ())), preferred_element_type=jnp.float32)
        for a, b in back
    )
    tiles = jnp.moveaxis(partial_value.reshape(2 * PAD, 4, D // 4), 1, 0)
    tiles = lax.all_to_all(tiles, "mp", 0, 0, tiled=True)
    ig = jnp.sum(tiles, axis=0).astype(jnp.bfloat16).reshape(2, PAD, D // 4)
    ig = jnp.where(core == 0, ig, ig[::-1])[:, :PATCHES]
    input_grad = ig.reshape(1, 2 * PATCHES, D // 4)

    images_all = 2 * nz * nx
    grad_up, square_up = totals[0, 0] / 2, totals[0, 1] / (2 * images_all)
    grad_down, square_down = totals[1, 0] / 2, totals[1, 1] / (2 * images_all)
    precision_new_up = (1.0 - average_rate) * precision_up + average_rate * square_up
    precision_new_down = (1.0 - average_rate) * precision_down + average_rate * square_down
    raw_up = grad_up / (precision_new_up + damping)
    raw_down = grad_down / (precision_new_down + damping)
    local = jnp.sum(raw_up * raw_up + raw_down * raw_down, axis=0, keepdims=True)
    local = jnp.sum(local.reshape(1, cols // 128, 128), axis=1, keepdims=True)
    group = nz * nx * 4
    everyone = lax.all_to_all(jnp.broadcast_to(local, (group, 1, 128)), ZXY, 0, 0, tiled=True)
    root_mean = jnp.sqrt(jnp.sum(everyone) / (2 * D * FF))
    factor = 1.0 / jnp.maximum(clip_level, root_mean)
    mean_new_up = mean_up - step_rate * factor * raw_up
    mean_new_down = mean_down - step_rate * factor * raw_down
    return (mean_new_up, precision_new_up, mean_new_down, precision_new_down, input_grad)


def solution(mesh):
    split = Mesh(
        mesh.devices.reshape(8, 4, mesh.shape["mp"], mesh.shape["mc"]), ("z", "x", "mp", "mc")
    )
    placed = (
        P(DP, None),
        P("mc", DP, None),
        P(DP, "mp"),
        P(DP, "mp"),
        P("mc", DP, "mp"),
        P(DP, "mp"),
        P(DP, "mp"),
        P("mc", DP, "mp"),
    )
    return jax.shard_map(
        shards,
        mesh=split,
        in_specs=placed,
        out_specs=(P(DP, "mp"), P(DP, "mp"), P(DP, "mp"), P(DP, "mp"), P("mc", DP, "mp")),
        check_vma=False,
    )
```

```python
import jax
import jax.numpy as jnp
from jax import lax
from jax.experimental import pallas as pl
from jax.experimental.pallas import tpu as pltpu
from jax.sharding import Mesh
from jax.sharding import PartitionSpec as P

D = 768
FF = 3072
PATCHES = 197
ROWS = 2 * PATCHES
HEAD = 208
TAIL = ROWS - HEAD
FULL = 400
HALF = D // 2
DP = ("z", "x")
ZXY = ("z", "x", "mp")

reciprocal_root = 0.7071067811865476
normal_peak = 0.3989422804014327
tempering = 100.0
damping = 4.0
average_rate = 0.25
step_rate = 0.05
clip_level = 0.01
square_unit = 256.0
grad_unit = 8.0

SMEM = pl.BlockSpec(memory_space=pltpu.SMEM)
VMEM = pl.BlockSpec(memory_space=pltpu.VMEM)


def shift(value, axis, k):
    n = lax.axis_size(axis)
    return lax.ppermute(value, axis, [(i, (i + k) % n) for i in range(n)])


def sample_kernel(mu_ref, pu_ref, nu_ref, md_ref, pd_ref, nd_ref, out_ref):
    nz, nx, _, width = out_ref.shape

    def drawn(m, p, n):
        spread = 1.0 / jnp.sqrt(tempering * (p[...] + damping))
        return m[...] + spread * n[...]

    up, down = drawn(mu_ref, pu_ref, nu_ref), drawn(md_ref, pd_ref, nd_ref)
    wide = width // 2
    for i in range(nx):
        cut = slice(i * wide, (i + 1) * wide)
        both = jnp.concatenate([up[:, cut], down[:, cut]], axis=1).astype(jnp.bfloat16)
        for k in range(nz):
            out_ref[k, i] = both


def dot_rows(left, right):
    return lax.dot_general(
        left, right, (((0,), (0,)), ((), ())), preferred_element_type=jnp.float32
    )


def groups_kernel(core_ref, wu_ref, wd_ref, *refs, groups, split, first):
    core = core_ref[0]
    per = 4 if split else 2
    ins, rest = refs[: per * groups], refs[per * groups :]
    if first:
        acc_in = None
    else:
        acc_in, rest = rest[0], rest[1:]
    acc, pg_refs, (f_s, c_s) = rest[0], rest[1 : 1 + groups], rest[1 + groups :]
    up_at, down_at = core, 1 - core
    row = lax.broadcasted_iota(jnp.int32, (HEAD, wu_ref.shape[1]), 0)
    for g in range(groups):
        f_s[HEAD + TAIL - 10 : FULL, :] = jnp.zeros((FULL - ROWS + 10, D), jnp.bfloat16)
        c_s[HEAD + TAIL - 10 : FULL, :] = jnp.zeros((FULL - ROWS + 10, D), jnp.bfloat16)
        if split:
            u0, u1, o0, o1 = ins[per * g : per * (g + 1)]
            f_s[0:HEAD, 0:HALF] = u0[:, 0:HALF]
            f_s[HEAD:ROWS, 0:HALF] = u1[:, 0:HALF]
            f_s[0:HEAD, HALF:D] = o0[...]
            f_s[HEAD:ROWS, HALF:D] = o1[...]
            c_s[0:HEAD, :] = u0[:, HALF:]
            c_s[HEAD:ROWS, :] = u1[:, HALF:]
            at = [core * HALF, (1 - core) * HALF]
            at = [pl.multiple_of(a, HALF) for a in at]
        else:
            f_ref, c_ref = ins[per * g : per * (g + 1)]
            f_s[0:ROWS, :] = f_ref[...]
            c_s[0:ROWS, :] = c_ref[...]
            at = [0, HALF]
        preact = sum(
            jnp.dot(
                f_s[:, i * HALF : (i + 1) * HALF],
                wu_ref[pl.ds(at[i], HALF), :],
                preferred_element_type=jnp.float32,
            )
            for i in range(2)
        )
        cumulative = 0.5 * (1.0 + lax.erf(preact * reciprocal_root))
        density = normal_peak * jnp.exp(-0.5 * preact * preact)
        hidden = (preact * cumulative).astype(jnp.bfloat16)
        back = jnp.dot(c_s[...], wd_ref[...], preferred_element_type=jnp.float32)
        pg = (back * (cumulative + preact * density)).astype(jnp.bfloat16)
        pg_refs[g][...] = pg[:ROWS]
        zero = jnp.zeros((), jnp.bfloat16)
        cuts = (slice(0, HEAD), slice(FULL - HEAD, FULL))
        keep = (row < PATCHES, row >= PATCHES - (FULL - HEAD))

        def add(index, at, source, lanes, right):
            each = [
                dot_rows(source[cut, lanes], jnp.where(k, right[cut], zero))
                for cut, k in zip(cuts, keep)
            ]
            total = each[0] + each[1]
            square = each[0] * each[0] + each[1] * each[1]
            span = pl.ds(at, HALF)
            if g == 0 and first:
                acc[index, 0, span, :] = total
                acc[index, 1, span, :] = square
            else:
                old = acc_in if g == 0 else acc
                acc[index, 0, span, :] = old[index, 0, span, :] + total
                acc[index, 1, span, :] = old[index, 1, span, :] + square

        for i in range(2):
            lanes = slice(i * HALF, (i + 1) * HALF)
            add(up_at, at[i], f_s, lanes, pg)
            add(down_at, i * HALF, c_s, lanes, hidden)


def run_groups(core, w_up, w_down, ins, acc, split):
    groups = len(ins) // (4 if split else 2)
    wide = w_up.shape[1]
    first = acc is None
    operands = [core, w_up, w_down, *ins] + ([] if first else [acc])
    kernel = lambda *refs: groups_kernel(*refs, groups=groups, split=split, first=first)
    flops = groups * ROWS * D * wide * 8
    return pl.pallas_call(
        kernel,
        out_shape=[jax.ShapeDtypeStruct((2, 2, D, wide), jnp.float32)]
        + [jax.ShapeDtypeStruct((ROWS, wide), jnp.bfloat16)] * groups,
        in_specs=[SMEM] + [VMEM] * (len(operands) - 1),
        out_specs=[VMEM] * (1 + groups),
        scratch_shapes=[pltpu.VMEM((FULL, D), jnp.bfloat16), pltpu.VMEM((FULL, D), jnp.bfloat16)],
        input_output_aliases={} if first else {len(operands) - 1: 0},
        cost_estimate=pl.CostEstimate(
            flops=flops, transcendentals=2 * groups * ROWS * wide, bytes_accessed=6 << 20
        ),
        name="groups%d" % groups + ("s" if split else ""),
    )(*operands)


def pack_kernel(mine_ref, other_ref, out_ref):
    rows = out_ref.shape[1]
    for k in range(0, out_ref.shape[0], 8):
        span = slice(k * rows, (k + 8) * rows)
        grad = mine_ref[0, span, :] + other_ref[0, span, :]
        square = mine_ref[1, span, :] + other_ref[1, span, :]
        root = jnp.sqrt(jnp.abs(grad)) * grad_unit
        both = jnp.concatenate(
            [jnp.where(grad < 0.0, -root, root), jnp.sqrt(square) * (1.0 / square_unit)], axis=1
        )
        out_ref[k : k + 8] = both.reshape(8, rows, both.shape[1])


def input_kernel(at_ref, *refs):
    pgs, ups, outs = refs[:4], refs[4:8], refs[8:]
    wide = outs[0].shape[1]
    for k, out in enumerate(outs):
        at = pl.multiple_of(((at_ref[0] + k) % len(outs)) * wide, wide)
        out[...] = sum(
            lax.dot_general(
                pg[...],
                up[pl.ds(at, wide), :],
                (((1,), (1,)), ((), ())),
                preferred_element_type=jnp.float32,
            )
            for pg, up in zip(pgs, ups)
        )


def shards(
    features, out_cotangent, mean_up, precision_up, noise_up, mean_down, precision_down, noise_down
):
    core = lax.axis_index("mc").astype(jnp.int32)
    nz, nx, ny = lax.axis_size("z"), lax.axis_size("x"), lax.axis_size("mp")
    rows, cols = mean_up.shape
    wide = cols // nx
    core_at = core.reshape(1)
    cotangent = out_cotangent[0]

    share = lax.dynamic_slice(features, (0, core * HALF), (ROWS, HALF))
    u0 = jnp.concatenate([share[:HEAD], cotangent[:HEAD]], axis=1)
    u1 = jnp.concatenate([share[HEAD:], cotangent[HEAD:]], axis=1)
    r0, l1 = shift(u0, "x", 1), shift(u1, "x", -1)

    payload = pl.pallas_call(
        sample_kernel,
        out_shape=jax.ShapeDtypeStruct((nz, nx, rows, 2 * wide), jnp.bfloat16),
        in_specs=[VMEM] * 6,
        out_specs=VMEM,
        name="sample",
    )(mean_up, precision_up, noise_up[0], mean_down, precision_down, noise_down[0])
    weights = lax.all_to_all(
        payload.reshape(nz * nx, rows, 2 * wide), DP, 0, 0, tiled=True
    ).reshape(D, 2 * wide)
    w_up, w_down = weights[:, :wide], weights[:, wide:]

    r1, l0 = shift(u1, "x", 1), shift(u0, "x", -1)
    f0, f1 = shift(r0, "x", 1), shift(l1, "x", -1)
    swap = lambda parts: shift(jnp.concatenate([p[:, :HALF] for p in parts], axis=0), "mc", 1)
    near = swap([r0, l0, r1, l1])
    far = swap([f0, f1])

    acc, pg = run_groups(core_at, w_up, w_down, [features, cotangent], None, False)
    near_in = [
        r0, r1, near[:HEAD], near[2 * HEAD : 2 * HEAD + TAIL],
        l0, l1, near[HEAD : 2 * HEAD], near[2 * HEAD + TAIL :],
    ]
    acc, pg_r, pg_l = run_groups(core_at, w_up, w_down, near_in, acc, True)
    acc, pg_f = run_groups(core_at, w_up, w_down, [f0, f1, far[:HEAD], far[HEAD:]], acc, True)

    traded = shift(acc[1], "mc", 1)
    packed = pl.pallas_call(
        pack_kernel,
        out_shape=jax.ShapeDtypeStruct((nz * nx, rows, 2 * wide), jnp.float32),
        in_specs=[VMEM] * 2,
        out_specs=VMEM,
        name="pack",
    )(acc[0], traded)
    got = lax.all_to_all(packed.astype(jnp.float16), DP, 0, 0, tiled=True)
    got = got.astype(jnp.float32).reshape(nz, nx, rows, 2, wide)
    part = lax.broadcasted_iota(jnp.int32, got.shape, 3)
    scale = jnp.where(part == 0, jnp.abs(got), got) * jnp.where(
        part == 0, 1.0 / (grad_unit * grad_unit), square_unit * square_unit
    )
    total = jnp.sum(got * scale, axis=0)
    total = jnp.transpose(total, (2, 1, 0, 3)).reshape(2, rows, cols)
    totals = lax.all_gather(total, "mc", axis=0)

    pgs = [pg, shift(pg_r, "x", -1), shift(pg_l, "x", 1), shift(pg_f, "x", 2)]
    ups = [w_up, shift(w_up, "x", -1), shift(w_up, "x", 1), shift(w_up, "x", 2)]
    tile = jax.ShapeDtypeStruct((ROWS, D // ny), jnp.float32)
    tiles = pl.pallas_call(
        input_kernel,
        out_shape=[tile] * ny,
        in_specs=[SMEM] + [VMEM] * 8,
        out_specs=[VMEM] * ny,
        cost_estimate=pl.CostEstimate(
            flops=ROWS * D * cols * 2, transcendentals=0, bytes_accessed=4 << 20
        ),
        name="input_grad",
    )(lax.axis_index("mp").astype(jnp.int32).reshape(1), *pgs, *ups)
    tiles = [tiles[0]] + [shift(tiles[k], "mp", k) for k in range(1, ny)]
    input_grad = sum(tiles[1:], tiles[0]).astype(jnp.bfloat16)[None]

    images_all = 2 * nz * nx
    grad_up, square_up = totals[0, 0] / 2, totals[0, 1] / (2 * images_all)
    grad_down, square_down = totals[1, 0] / 2, totals[1, 1] / (2 * images_all)
    precision_new_up = (1.0 - average_rate) * precision_up + average_rate * square_up
    precision_new_down = (1.0 - average_rate) * precision_down + average_rate * square_down
    raw_up = grad_up / (precision_new_up + damping)
    raw_down = grad_down / (precision_new_down + damping)
    local = jnp.sum(raw_up * raw_up + raw_down * raw_down, axis=0, keepdims=True)
    local = jnp.sum(local.reshape(1, cols // 128, 128), axis=1, keepdims=True)
    group = nz * nx * ny
    everyone = lax.all_to_all(jnp.broadcast_to(local, (group, 1, 128)), ZXY, 0, 0, tiled=True)
    root_mean = jnp.sqrt(jnp.sum(everyone) / (2 * D * FF))
    factor = 1.0 / jnp.maximum(clip_level, root_mean)
    mean_new_up = mean_up - step_rate * factor * raw_up
    mean_new_down = mean_down - step_rate * factor * raw_down
    return (mean_new_up, precision_new_up, mean_new_down, precision_new_down, input_grad)


def solution(mesh):
    split = Mesh(
        mesh.devices.reshape(8, 4, mesh.shape["mp"], mesh.shape["mc"]), ("z", "x", "mp", "mc")
    )
    placed = (
        P(DP, None),
        P("mc", DP, None),
        P(DP, "mp"),
        P(DP, "mp"),
        P("mc", DP, "mp"),
        P(DP, "mp"),
        P(DP, "mp"),
        P("mc", DP, "mp"),
    )
    return jax.shard_map(
        shards,
        mesh=split,
        in_specs=placed,
        out_specs=(P(DP, "mp"), P(DP, "mp"), P(DP, "mp"), P(DP, "mp"), P("mc", DP, "mp")),
        check_vma=False,
    )
```

```python
import jax
import jax.numpy as jnp
from jax import lax
from jax.experimental import pallas as pl
from jax.experimental.pallas import tpu as pltpu
from jax.sharding import Mesh
from jax.sharding import PartitionSpec as P


D = 768
FF = 3072
PATCHES = 197
ROWS = 2 * PATCHES
HEAD = 208
TAIL = ROWS - HEAD
FULL = 400
HALF = D // 2
DP = ("z", "x")
ZXY = ("z", "x", "mp")

reciprocal_root = 0.7071067811865476
normal_peak = 0.3989422804014327
tempering = 100.0
damping = 4.0
average_rate = 0.25
step_rate = 0.05
clip_level = 0.01
square_unit = 256.0
grad_unit = 8.0

SMEM = pl.BlockSpec(memory_space=pltpu.SMEM)
VMEM = pl.BlockSpec(memory_space=pltpu.VMEM)


def shift(value, axis, k):
    n = lax.axis_size(axis)
    return lax.ppermute(value, axis, [(i, (i + k) % n) for i in range(n)])


def sample_kernel(mu_ref, pu_ref, nu_ref, md_ref, pd_ref, nd_ref, out_ref):
    nz, nx, _, width = out_ref.shape

    def drawn(m, p, n):
        spread = 1.0 / jnp.sqrt(tempering * (p[...] + damping))
        return m[...] + spread * n[...]

    up, down = drawn(mu_ref, pu_ref, nu_ref), drawn(md_ref, pd_ref, nd_ref)
    wide = width // 2
    for i in range(nx):
        cut = slice(i * wide, (i + 1) * wide)
        both = jnp.concatenate([up[:, cut], down[:, cut]], axis=1).astype(jnp.bfloat16)
        for k in range(nz):
            out_ref[k, i] = both


def stage_kernel(core_ref, f_ref, c_ref, head_ref, tail_ref):
    first = core_ref[0] == 0
    for out, cut in ((head_ref, slice(0, HEAD)), (tail_ref, slice(HEAD, ROWS))):
        out[:, 0:HALF] = jnp.where(first, f_ref[cut, 0:HALF], f_ref[cut, HALF:D])
        out[:, HALF:] = c_ref[cut, :]


def dot_rows(left, right):
    return lax.dot_general(
        left, right, (((0,), (0,)), ((), ())), preferred_element_type=jnp.float32
    )


def pack_lanes(value, rows):
    return jnp.concatenate([value[:rows], value[value.shape[0] - rows :]], axis=1)


def groups_kernel(core_ref, wu_ref, wd_ref, *refs, swapped, last):
    core = core_ref[0]
    if last:
        u0, u1, near, acc_in = refs[:4]
        mine_ref, other_ref, parcel, f_s, c_s, acc = refs[4:]
        pairs = [(u0, u1, swapped[0], parcel)]
    else:
        f_ref, c_ref, r0, r1, l0, l1, near = refs[:7]
        acc, pg_ref, parcel_r, parcel_l, f_s, c_s = refs[7:]
        acc_in = None
        pairs = [
            (None, None, None, pg_ref),
            (r0, r1, swapped[0], parcel_r),
            (l0, l1, swapped[1], parcel_l),
        ]
    up_at, down_at = core, 1 - core
    wide = wu_ref.shape[1]
    row = lax.broadcasted_iota(jnp.int32, (HEAD, wide), 0)
    f_s[FULL - 16 : FULL, :] = jnp.zeros((16, D), jnp.bfloat16)
    c_s[FULL - 16 : FULL, :] = jnp.zeros((16, D), jnp.bfloat16)
    for g, (u0, u1, spots, out) in enumerate(pairs):
        if u0 is None:
            f_s[0:ROWS, :] = f_ref[...]
            c_s[0:ROWS, :] = c_ref[...]
            at = [0, HALF]
        else:
            f_s[0:HEAD, 0:HALF] = u0[:, 0:HALF]
            f_s[HEAD:ROWS, 0:HALF] = u1[:, 0:HALF]
            f_s[0:HEAD, HALF:D] = near[spots[0] : spots[0] + HEAD, :]
            f_s[HEAD:ROWS, HALF:D] = near[spots[1] : spots[1] + TAIL, :]
            c_s[0:HEAD, :] = u0[:, HALF:]
            c_s[HEAD:ROWS, :] = u1[:, HALF:]
            at = [pl.multiple_of(a, HALF) for a in (core * HALF, (1 - core) * HALF)]
        preact = sum(
            jnp.dot(
                f_s[:, i * HALF : (i + 1) * HALF],
                wu_ref[pl.ds(at[i], HALF), :],
                preferred_element_type=jnp.float32,
            )
            for i in range(2)
        )
        cumulative = 0.5 * (1.0 + lax.erf(preact * reciprocal_root))
        density = normal_peak * jnp.exp(-0.5 * preact * preact)
        hidden = (preact * cumulative).astype(jnp.bfloat16)
        back = jnp.dot(c_s[...], wd_ref[...], preferred_element_type=jnp.float32)
        pg = (back * (cumulative + preact * density)).astype(jnp.bfloat16)
        if u0 is None:
            out[...] = pg[:ROWS]
        else:
            out[0:HALF, :] = pack_lanes(wu_ref[...], HALF)
            out[HALF:, :] = pack_lanes(pg, HEAD)
        zero = jnp.zeros((), jnp.bfloat16)
        cuts = (slice(0, HEAD), slice(FULL - HEAD, FULL))
        keep = (row < PATCHES, row >= PATCHES - (FULL - HEAD))

        def add(index, at, source, lanes, right):
            each = [dot_rows(source[cut, lanes], right[i]) for i, cut in enumerate(cuts)]
            total = jnp.concatenate(
                [each[0] + each[1], each[0] * each[0] + each[1] * each[1]], axis=1
            )
            span = pl.ds(at, HALF)
            if g == 0 and last:
                acc[index, span, :] = acc_in[index, span, :] + total
            elif g == 0:
                acc[index, span, :] = total
            else:
                acc[index, span, :] = acc[index, span, :] + total

        by_image = [
            [jnp.where(k, v[cut], zero) for cut, k in zip(cuts, keep)] for v in (pg, hidden)
        ]
        for i in range(2):
            lanes = slice(i * HALF, (i + 1) * HALF)
            add(up_at, at[i], f_s, lanes, by_image[0])
            add(down_at, i * HALF, c_s, lanes, by_image[1])
    if last:
        mine_ref[...] = acc[0]
        other_ref[...] = acc[1]


def run_groups(core, w_up, w_down, ins, swapped, last):
    wide = w_up.shape[1]
    sums = jax.ShapeDtypeStruct((D, 2 * wide), jnp.float32)
    parcel = jax.ShapeDtypeStruct((HALF + HEAD, 2 * wide), jnp.bfloat16)
    pair = pltpu.VMEM((FULL, D), jnp.bfloat16)
    if last:
        out_shape, scratch = [sums, sums, parcel], [pltpu.VMEM((2, D, 2 * wide), jnp.float32)]
    else:
        out_shape = [
            jax.ShapeDtypeStruct((2, D, 2 * wide), jnp.float32),
            jax.ShapeDtypeStruct((ROWS, wide), jnp.bfloat16),
            parcel,
            parcel,
        ]
        scratch = []
    groups = 1 if last else 3
    return pl.pallas_call(
        lambda *refs: groups_kernel(*refs, swapped=swapped, last=last),
        out_shape=out_shape,
        in_specs=[SMEM] + [VMEM] * (len(ins) + 2),
        out_specs=[VMEM] * len(out_shape),
        scratch_shapes=[pair, pair] + scratch,
        cost_estimate=pl.CostEstimate(
            flops=groups * ROWS * D * wide * 8,
            transcendentals=2 * groups * ROWS * wide,
            bytes_accessed=6 << 20,
        ),
    )(core, w_up, w_down, *ins)


def input_kernel(at_ref, pg_ref, up_ref, *refs):
    parcels, outs, (up_s, pg_s) = refs[:3], refs[3:-2], refs[-2:]
    wide = pg_ref.shape[1]
    for i, parcel in enumerate(parcels):
        up_s[i, 0:HALF] = parcel[0:HALF, 0:wide]
        up_s[i, HALF:D] = parcel[0:HALF, wide:]
        pg_s[i, 0:HEAD] = parcel[HALF:, 0:wide]
        pg_s[i, FULL - HEAD : FULL] = parcel[HALF:, wide:]
    for k, out in enumerate(outs):
        at = pl.multiple_of(((at_ref[0] + k) % len(outs)) * wide, wide)
        span = pl.ds(at, wide)

        def product(left, right):
            return lax.dot_general(
                left, right, (((1,), (1,)), ((), ())), preferred_element_type=jnp.float32
            )

        value = product(pg_ref[...], up_ref[span, :])
        for i in range(len(parcels)):
            value = value + product(pg_s[i, 0:ROWS], up_s[i, span, :])
        out[...] = value


def shards(
    features, out_cotangent, mean_up, precision_up, noise_up, mean_down, precision_down, noise_down
):
    core = lax.axis_index("mc").astype(jnp.int32)
    nz, nx, ny = lax.axis_size("z"), lax.axis_size("x"), lax.axis_size("mp")
    rows, cols = mean_up.shape
    wide = cols // nx
    core_at = core.reshape(1)
    cotangent = out_cotangent[0]

    u0, u1 = pl.pallas_call(
        stage_kernel,
        out_shape=[
            jax.ShapeDtypeStruct((HEAD, HALF + D), jnp.bfloat16),
            jax.ShapeDtypeStruct((TAIL, HALF + D), jnp.bfloat16),
        ],
        in_specs=[SMEM, VMEM, VMEM],
        out_specs=[VMEM, VMEM],
        name="stage",
    )(core_at, features, cotangent)
    r0 = shift(u0, "x", 1)
    l1 = shift(u1, "x", -1)
    r1 = shift(u1, "x", 1)
    l0 = shift(u0, "x", -1)

    payload = pl.pallas_call(
        sample_kernel,
        out_shape=jax.ShapeDtypeStruct((nz, nx, rows, 2 * wide), jnp.bfloat16),
        in_specs=[VMEM] * 6,
        out_specs=VMEM,
        name="sample",
    )(mean_up, precision_up, noise_up[0], mean_down, precision_down, noise_down[0])
    weights = lax.all_to_all(
        payload.reshape(nz * nx, rows, 2 * wide), DP, 0, 0, tiled=True
    ).reshape(D, 2 * wide)
    w_up, w_down = weights[:, :wide], weights[:, wide:]

    f0 = shift(r0, "x", 1)
    f1 = shift(l1, "x", -1)
    gap = jnp.zeros((FULL - HEAD - TAIL, HALF), jnp.bfloat16)
    near = jnp.concatenate([r0[:, :HALF], l0[:, :HALF], r1[:, :HALF], gap, l1[:, :HALF]])
    near = shift(near, "mc", 1)
    spots = ((0, 2 * HEAD), (HEAD, HEAD + FULL))
    far = shift(jnp.concatenate([f0[:, :HALF], f1[:, :HALF]]), "mc", 1)

    acc, pg, parcel_r, parcel_l = run_groups(
        core_at, w_up, w_down, [features, cotangent, r0, r1, l0, l1, near], spots, False
    )
    parcel_r = shift(parcel_r, "x", -1)
    parcel_l = shift(parcel_l, "x", 1)
    mine, other, parcel_f = run_groups(
        core_at, w_up, w_down, [f0, f1, far, acc], ((0, HEAD),), True
    )

    both = mine + shift(other, "mc", 1)
    parcel_f = shift(parcel_f, "x", 2)
    is_grad = lax.broadcasted_iota(jnp.int32, both.shape, 1) < wide
    root = jnp.sqrt(jnp.abs(both)) * jnp.where(is_grad, grad_unit, 1.0 / square_unit)
    packed = jnp.where(both < 0.0, -root, root).astype(jnp.float16)
    got = lax.all_to_all(packed.reshape(nz * nx, rows, 2 * wide), DP, 0, 0, tiled=True)
    got = got.astype(jnp.float32).reshape(nz, nx, rows, 2 * wide)
    is_grad = lax.broadcasted_iota(jnp.int32, got.shape, 3) < wide
    got = jnp.where(
        is_grad, got * jnp.abs(got) / (grad_unit * grad_unit), (square_unit * got) * (square_unit * got)
    )
    total = jnp.sum(got, axis=0).reshape(nx, rows, 2, wide)
    total = jnp.transpose(total, (2, 1, 0, 3)).reshape(2, rows, cols)
    totals = lax.all_gather(total, "mc", axis=0)

    tile = jax.ShapeDtypeStruct((ROWS, D // ny), jnp.float32)
    tiles = pl.pallas_call(
        input_kernel,
        out_shape=[tile] * ny,
        in_specs=[SMEM] + [VMEM] * 5,
        out_specs=[VMEM] * ny,
        scratch_shapes=[
            pltpu.VMEM((3, D, wide), jnp.bfloat16),
            pltpu.VMEM((3, FULL, wide), jnp.bfloat16),
        ],
        cost_estimate=pl.CostEstimate(
            flops=ROWS * D * cols * 2, transcendentals=0, bytes_accessed=4 << 20
        ),
        name="input_grad",
    )(lax.axis_index("mp").astype(jnp.int32).reshape(1), pg, w_up, parcel_r, parcel_l, parcel_f)
    tiles = [tiles[0]] + [shift(tiles[k], "mp", k) for k in range(1, ny)]
    input_grad = sum(tiles[1:], tiles[0]).astype(jnp.bfloat16)[None]

    images_all = 2 * nz * nx
    grad_up, square_up = totals[0, 0] / 2, totals[0, 1] / (2 * images_all)
    grad_down, square_down = totals[1, 0] / 2, totals[1, 1] / (2 * images_all)
    precision_new_up = (1.0 - average_rate) * precision_up + average_rate * square_up
    precision_new_down = (1.0 - average_rate) * precision_down + average_rate * square_down
    raw_up = grad_up / (precision_new_up + damping)
    raw_down = grad_down / (precision_new_down + damping)
    local = jnp.sum(raw_up * raw_up + raw_down * raw_down, axis=0, keepdims=True)
    local = jnp.sum(local.reshape(1, cols // 128, 128), axis=1, keepdims=True)
    group = nz * nx * ny
    everyone = lax.all_to_all(jnp.broadcast_to(local, (group, 1, 128)), ZXY, 0, 0, tiled=True)
    root_mean = jnp.sqrt(jnp.sum(everyone) / (2 * D * FF))
    factor = 1.0 / jnp.maximum(clip_level, root_mean)
    mean_new_up = mean_up - step_rate * factor * raw_up
    mean_new_down = mean_down - step_rate * factor * raw_down
    return (mean_new_up, precision_new_up, mean_new_down, precision_new_down, input_grad)


def solution(mesh):
    split = Mesh(
        mesh.devices.reshape(8, 4, mesh.shape["mp"], mesh.shape["mc"]), ("z", "x", "mp", "mc")
    )
    placed = (
        P(DP, None),
        P("mc", DP, None),
        P(DP, "mp"),
        P(DP, "mp"),
        P("mc", DP, "mp"),
        P(DP, "mp"),
        P(DP, "mp"),
        P("mc", DP, "mp"),
    )

    def step(*args):
        return shards(*args)

    step = jax.shard_map(
        step,
        mesh=split,
        in_specs=placed,
        out_specs=(P(DP, "mp"), P(DP, "mp"), P(DP, "mp"), P(DP, "mp"), P("mc", DP, "mp")),
        check_vma=False,
    )
    return step
```

```python
import jax
import jax.numpy as jnp
from jax import lax
from jax.experimental import pallas as pl
from jax.experimental.pallas import tpu as pltpu
from jax.sharding import Mesh
from jax.sharding import PartitionSpec as P


D = 768
FF = 3072
PATCHES = 197
ROWS = 2 * PATCHES
HEAD = 208
TAIL = ROWS - HEAD
FULL = 400
HALF = D // 2
DP = ("z", "x")
ZXY = ("z", "x", "mp")

reciprocal_root = 0.7071067811865476
normal_peak = 0.3989422804014327
tempering = 100.0
damping = 4.0
average_rate = 0.25
step_rate = 0.05
clip_level = 0.01
square_unit = 256.0
grad_unit = 8.0

SMEM = pl.BlockSpec(memory_space=pltpu.SMEM)
VMEM = pl.BlockSpec(memory_space=pltpu.VMEM)


def shift(value, axis, k):
    n = lax.axis_size(axis)
    return lax.ppermute(value, axis, [(i, (i + k) % n) for i in range(n)])


def prepare_kernel(
    core_ref, f_ref, c_ref, mu_ref, pu_ref, nu_ref, md_ref, pd_ref, nd_ref, head_ref, tail_ref, w_ref
):
    first = core_ref[0] == 0
    for out, cut in ((head_ref, slice(0, HEAD)), (tail_ref, slice(HEAD, ROWS))):
        out[:, 0:HALF] = jnp.where(first, f_ref[cut, 0:HALF], f_ref[cut, HALF:D])
        out[:, HALF:] = c_ref[cut, :]
    nz, nx, _, width = w_ref.shape

    def drawn(m, p, n):
        spread = 1.0 / jnp.sqrt(tempering * (p[...] + damping))
        return m[...] + spread * n[...]

    up, down = drawn(mu_ref, pu_ref, nu_ref), drawn(md_ref, pd_ref, nd_ref)
    wide = width // 2
    for i in range(nx):
        cut = slice(i * wide, (i + 1) * wide)
        both = jnp.concatenate([up[:, cut], down[:, cut]], axis=1).astype(jnp.bfloat16)
        for k in range(nz):
            w_ref[k, i] = both


def dot_rows(left, right):
    return lax.dot_general(
        left, right, (((0,), (0,)), ((), ())), preferred_element_type=jnp.float32
    )


def gather_kernel(*refs):
    at = 0
    for ref in refs[:-1]:
        refs[-1][at : at + ref.shape[0], :] = ref[:, 0:HALF]
        at += -(-ref.shape[0] // 16) * 16


def pack_lanes(value, rows):
    return jnp.concatenate([value[:rows], value[value.shape[0] - rows :]], axis=1)


def groups_kernel(core_ref, w_ref, *refs, swapped, last):
    core = core_ref[0]
    if last:
        u0, u1, near, acc_in = refs[:4]
        mine_ref, other_ref, parcel, f_s, c_s, wd_ref, acc = refs[4:]
        pairs = [(u0, u1, swapped[0], parcel)]
    else:
        f_ref, c_ref, r0, r1, l0, l1, near = refs[:7]
        acc, pg_ref, parcel_r, parcel_l, f_s, c_s, wd_ref = refs[7:]
        acc_in = None
        pairs = [
            (None, None, None, pg_ref),
            (r0, r1, swapped[0], parcel_r),
            (l0, l1, swapped[1], parcel_l),
        ]
    up_at, down_at = core, 1 - core
    wide = w_ref.shape[1] // 2
    wd_ref[...] = w_ref[:, wide:]
    row = lax.broadcasted_iota(jnp.int32, (HEAD, wide), 0)
    f_s[FULL - 16 : FULL, :] = jnp.zeros((16, D), jnp.bfloat16)
    c_s[FULL - 16 : FULL, :] = jnp.zeros((16, D), jnp.bfloat16)
    for g, (u0, u1, spots, out) in enumerate(pairs):
        if u0 is None:
            f_s[0:ROWS, :] = f_ref[...]
            c_s[0:ROWS, :] = c_ref[...]
            at = [0, HALF]
        else:
            f_s[0:HEAD, 0:HALF] = u0[:, 0:HALF]
            f_s[HEAD:ROWS, 0:HALF] = u1[:, 0:HALF]
            f_s[0:HEAD, HALF:D] = near[spots[0] : spots[0] + HEAD, :]
            f_s[HEAD:ROWS, HALF:D] = near[spots[1] : spots[1] + TAIL, :]
            c_s[0:HEAD, :] = u0[:, HALF:]
            c_s[HEAD:ROWS, :] = u1[:, HALF:]
            at = [pl.multiple_of(a, HALF) for a in (core * HALF, (1 - core) * HALF)]
        preact = sum(
            jnp.dot(
                f_s[:, i * HALF : (i + 1) * HALF],
                w_ref[pl.ds(at[i], HALF), 0:wide],
                preferred_element_type=jnp.float32,
            )
            for i in range(2)
        )
        cumulative = 0.5 * (1.0 + lax.erf(preact * reciprocal_root))
        density = normal_peak * jnp.exp(-0.5 * preact * preact)
        hidden = (preact * cumulative).astype(jnp.bfloat16)
        back = jnp.dot(c_s[...], wd_ref[...], preferred_element_type=jnp.float32)
        pg = (back * (cumulative + preact * density)).astype(jnp.bfloat16)
        if u0 is None:
            out[...] = pg[:ROWS]
        else:
            out[0:HALF, :] = pack_lanes(w_ref[:, 0:wide], HALF)
            out[HALF:, :] = pack_lanes(pg, HEAD)
        zero = jnp.zeros((), jnp.bfloat16)
        cuts = (slice(0, HEAD), slice(FULL - HEAD, FULL))
        keep = (row < PATCHES, row >= PATCHES - (FULL - HEAD))

        def add(index, at, source, lanes, right):
            each = [dot_rows(source[cut, lanes], right[i]) for i, cut in enumerate(cuts)]
            total = jnp.concatenate(
                [each[0] + each[1], each[0] * each[0] + each[1] * each[1]], axis=1
            )
            span = pl.ds(at, HALF)
            if g == 0 and last:
                acc[index, span, :] = acc_in[index, span, :] + total
            elif g == 0:
                acc[index, span, :] = total
            else:
                acc[index, span, :] = acc[index, span, :] + total

        by_image = [
            [jnp.where(k, v[cut], zero) for cut, k in zip(cuts, keep)] for v in (pg, hidden)
        ]
        for i in range(2):
            lanes = slice(i * HALF, (i + 1) * HALF)
            add(up_at, at[i], f_s, lanes, by_image[0])
            add(down_at, i * HALF, c_s, lanes, by_image[1])
    if last:
        mine_ref[...] = acc[0]
        other_ref[...] = acc[1]


def inside(array):
    return pltpu.with_memory_space_constraint(array, pltpu.VMEM)


def gathered(parts):
    return pl.pallas_call(
        gather_kernel,
        out_shape=pltpu.VMEM((sum(-(-p.shape[0] // 16) * 16 for p in parts), HALF), jnp.bfloat16),
        in_specs=[VMEM] * len(parts),
        out_specs=VMEM,
        compiler_params=pltpu.CompilerParams(vmem_limit_bytes=4 << 20),
    )(*map(inside, parts))


def run_groups(core, weights, ins, swapped, last):
    wide = weights.shape[1] // 2
    sums = pltpu.VMEM((D, 2 * wide), jnp.float32)
    parcel = pltpu.VMEM((HALF + HEAD, 2 * wide), jnp.bfloat16)
    pair = pltpu.VMEM((FULL, D), jnp.bfloat16)
    scratch = [pair, pair, pltpu.VMEM((D, wide), jnp.bfloat16)]
    if last:
        out_shape = [sums, sums, parcel]
        scratch.append(pltpu.VMEM((2, D, 2 * wide), jnp.float32))
    else:
        out_shape = [
            pltpu.VMEM((2, D, 2 * wide), jnp.float32),
            pltpu.VMEM((ROWS, wide), jnp.bfloat16),
            parcel,
            parcel,
        ]
    groups = 1 if last else 3
    return pl.pallas_call(
        lambda *refs: groups_kernel(*refs, swapped=swapped, last=last),
        out_shape=out_shape,
        in_specs=[SMEM] + [VMEM] * (len(ins) + 1),
        out_specs=[VMEM] * len(out_shape),
        scratch_shapes=scratch,
        compiler_params=pltpu.CompilerParams(vmem_limit_bytes=24 << 20),
        cost_estimate=pl.CostEstimate(
            flops=groups * ROWS * D * wide * 8,
            transcendentals=2 * groups * ROWS * wide,
            bytes_accessed=6 << 20,
        ),
    )(core, inside(weights), *[inside(a) for a in ins])


def input_kernel(at_ref, pg_ref, w_ref, *refs):
    parcels, outs, (up_s, pg_s) = refs[:3], refs[3:-2], refs[-2:]
    wide = pg_ref.shape[1]
    for i, parcel in enumerate(parcels):
        up_s[i, 0:HALF] = parcel[0:HALF, 0:wide]
        up_s[i, HALF:D] = parcel[0:HALF, wide:]
        pg_s[i, 0:HEAD] = parcel[HALF:, 0:wide]
        pg_s[i, FULL - HEAD : FULL] = parcel[HALF:, wide:]
    for k, out in enumerate(outs):
        at = pl.multiple_of(((at_ref[0] + k) % len(outs)) * wide, wide)
        span = pl.ds(at, wide)

        def product(left, right):
            return lax.dot_general(
                left, right, (((1,), (1,)), ((), ())), preferred_element_type=jnp.float32
            )

        value = product(pg_ref[...], w_ref[span, 0:wide])
        for i in range(len(parcels)):
            value = value + product(pg_s[i, 0:ROWS], up_s[i, span, :])
        out[...] = value


def shards(
    features, out_cotangent, mean_up, precision_up, noise_up, mean_down, precision_down, noise_down
):
    core = lax.axis_index("mc").astype(jnp.int32)
    nz, nx, ny = lax.axis_size("z"), lax.axis_size("x"), lax.axis_size("mp")
    rows, cols = mean_up.shape
    wide = cols // nx
    core_at = core.reshape(1)
    cotangent = out_cotangent[0]

    u0, u1, payload = pl.pallas_call(
        prepare_kernel,
        out_shape=[
            pltpu.VMEM((HEAD, HALF + D), jnp.bfloat16),
            pltpu.VMEM((TAIL, HALF + D), jnp.bfloat16),
            pltpu.VMEM((nz, nx, rows, 2 * wide), jnp.bfloat16),
        ],
        in_specs=[SMEM] + [VMEM] * 8,
        out_specs=[VMEM] * 3,
        compiler_params=pltpu.CompilerParams(vmem_limit_bytes=16 << 20),
        name="prepare",
    )(
        core_at,
        *[
            pltpu.with_memory_space_constraint(a, pltpu.HBM)
            for a in (
                features, cotangent, mean_up, precision_up, noise_up[0],
                mean_down, precision_down, noise_down[0],
            )
        ],
    )
    r0 = shift(u0, "x", 1)
    l1 = shift(u1, "x", -1)
    r1 = shift(u1, "x", 1)
    l0 = shift(u0, "x", -1)

    weights = lax.all_to_all(
        payload.reshape(nz * nx, rows, 2 * wide), DP, 0, 0, tiled=True
    ).reshape(D, 2 * wide)

    f0 = shift(r0, "x", 1)
    f1 = shift(l1, "x", -1)
    near = gathered([r0, l0, r1, l1])
    near = shift(near, "mc", 1)
    spots = ((0, 2 * HEAD), (HEAD, HEAD + FULL))
    far = shift(gathered([f0, f1]), "mc", 1)

    acc, pg, parcel_r, parcel_l = run_groups(
        core_at, weights, [features, cotangent, r0, r1, l0, l1, near], spots, False
    )
    parcel_r = shift(parcel_r, "x", -1)
    parcel_l = shift(parcel_l, "x", 1)
    mine, other, parcel_f = run_groups(
        core_at, weights, [f0, f1, far, acc], ((0, HEAD),), True
    )

    both = mine + shift(other, "mc", 1)
    parcel_f = shift(parcel_f, "x", 2)
    is_grad = lax.broadcasted_iota(jnp.int32, both.shape, 1) < wide
    root = jnp.sqrt(jnp.abs(both)) * jnp.where(is_grad, grad_unit, 1.0 / square_unit)
    packed = jnp.where(both < 0.0, -root, root).astype(jnp.float16)
    got = lax.all_to_all(packed.reshape(nz * nx, rows, 2 * wide), DP, 0, 0, tiled=True)
    got = got.astype(jnp.float32).reshape(nz, nx, rows, 2 * wide)
    is_grad = lax.broadcasted_iota(jnp.int32, got.shape, 3) < wide
    got = jnp.where(
        is_grad, got * jnp.abs(got) / (grad_unit * grad_unit), (square_unit * got) * (square_unit * got)
    )
    total = jnp.sum(got, axis=0).reshape(nx, rows, 2, wide)
    total = jnp.transpose(total, (2, 1, 0, 3)).reshape(2, rows, cols)
    totals = lax.all_gather(total, "mc", axis=0)

    tile = pltpu.VMEM((ROWS, D // ny), jnp.float32)
    tiles = pl.pallas_call(
        input_kernel,
        out_shape=[tile] * ny,
        in_specs=[SMEM] + [VMEM] * 5,
        out_specs=[VMEM] * ny,
        scratch_shapes=[
            pltpu.VMEM((3, D, wide), jnp.bfloat16),
            pltpu.VMEM((3, FULL, wide), jnp.bfloat16),
        ],
        compiler_params=pltpu.CompilerParams(vmem_limit_bytes=16 << 20),
        cost_estimate=pl.CostEstimate(
            flops=ROWS * D * cols * 2, transcendentals=0, bytes_accessed=4 << 20
        ),
        name="input_grad",
    )(lax.axis_index("mp").astype(jnp.int32).reshape(1), *map(inside, (pg, weights, parcel_r, parcel_l, parcel_f)))
    tiles = [tiles[0]] + [shift(tiles[k], "mp", k) for k in range(1, ny)]
    input_grad = sum(tiles[1:], tiles[0]).astype(jnp.bfloat16)[None]

    images_all = 2 * nz * nx
    grad_up, square_up = totals[0, 0] / 2, totals[0, 1] / (2 * images_all)
    grad_down, square_down = totals[1, 0] / 2, totals[1, 1] / (2 * images_all)
    precision_new_up = (1.0 - average_rate) * precision_up + average_rate * square_up
    precision_new_down = (1.0 - average_rate) * precision_down + average_rate * square_down
    raw_up = grad_up / (precision_new_up + damping)
    raw_down = grad_down / (precision_new_down + damping)
    local = jnp.sum(raw_up * raw_up + raw_down * raw_down, axis=0, keepdims=True)
    local = jnp.sum(local.reshape(1, cols // 128, 128), axis=1, keepdims=True)
    group = nz * nx * ny
    everyone = lax.all_to_all(jnp.broadcast_to(local, (group, 1, 128)), ZXY, 0, 0, tiled=True)
    root_mean = jnp.sqrt(jnp.sum(everyone) / (2 * D * FF))
    factor = 1.0 / jnp.maximum(clip_level, root_mean)
    mean_new_up = mean_up - step_rate * factor * raw_up
    mean_new_down = mean_down - step_rate * factor * raw_down
    return (mean_new_up, precision_new_up, mean_new_down, precision_new_down, input_grad)


def solution(mesh):
    split = Mesh(
        mesh.devices.reshape(8, 4, mesh.shape["mp"], mesh.shape["mc"]), ("z", "x", "mp", "mc")
    )
    placed = (
        P(DP, None),
        P("mc", DP, None),
        P(DP, "mp"),
        P(DP, "mp"),
        P("mc", DP, "mp"),
        P(DP, "mp"),
        P(DP, "mp"),
        P("mc", DP, "mp"),
    )

    def step(*args):
        return shards(*args)

    step = jax.shard_map(
        step,
        mesh=split,
        in_specs=placed,
        out_specs=(P(DP, "mp"), P(DP, "mp"), P(DP, "mp"), P(DP, "mp"), P("mc", DP, "mp")),
        check_vma=False,
    )
    return step
```

```python
import jax
import jax.numpy as jnp
from jax import lax
from jax.experimental import pallas as pl
from jax.experimental.pallas import tpu as pltpu
from jax.sharding import Mesh
from jax.sharding import PartitionSpec as P


D = 768
FF = 3072
PATCHES = 197
ROWS = 2 * PATCHES
HEAD = 208
TAIL = ROWS - HEAD
FULL = 400
HALF = D // 2
DP = ("z", "x")
ZXY = ("z", "x", "mp")

reciprocal_root = 0.7071067811865476
normal_peak = 0.3989422804014327
tempering = 100.0
damping = 4.0
average_rate = 0.25
step_rate = 0.05
clip_level = 0.01
square_unit = 256.0
grad_unit = 8.0

SMEM = pl.BlockSpec(memory_space=pltpu.SMEM)
VMEM = pl.BlockSpec(memory_space=pltpu.VMEM)
ANY = pl.BlockSpec(memory_space=pl.ANY)


def shift(value, axis, k):
    n = lax.axis_size(axis)
    return lax.ppermute(value, axis, [(i, (i + k) % n) for i in range(n)])


def prepare_kernel(
    core_ref, f_ref, c_ref, mu_ref, pu_ref, nu_ref, md_ref, pd_ref, nd_ref, head_ref, tail_ref, w_ref
):
    first = core_ref[0] == 0
    for out, cut in ((head_ref, slice(0, HEAD)), (tail_ref, slice(HEAD, ROWS))):
        out[:, 0:HALF] = jnp.where(first, f_ref[cut, 0:HALF], f_ref[cut, HALF:D])
        out[:, HALF:] = c_ref[cut, :]
    nz, nx, _, width = w_ref.shape

    def drawn(m, p, n):
        spread = 1.0 / jnp.sqrt(tempering * (p[...] + damping))
        return m[...] + spread * n[...]

    up, down = drawn(mu_ref, pu_ref, nu_ref), drawn(md_ref, pd_ref, nd_ref)
    wide = width // 2
    for i in range(nx):
        cut = slice(i * wide, (i + 1) * wide)
        both = jnp.concatenate([up[:, cut], down[:, cut]], axis=1).astype(jnp.bfloat16)
        for k in range(nz):
            w_ref[k, i] = both


def dot_rows(left, right):
    return lax.dot_general(
        left, right, (((0,), (0,)), ((), ())), preferred_element_type=jnp.float32
    )


def gather_kernel(*refs):
    at = 0
    for ref in refs[:-1]:
        refs[-1][at : at + ref.shape[0], :] = ref[:, 0:HALF]
        at += -(-ref.shape[0] // 16) * 16


def pack_lanes(value, rows):
    return jnp.concatenate([value[:rows], value[value.shape[0] - rows :]], axis=1)


def groups_kernel(core_ref, w_ref, *refs, swapped, last):
    core = core_ref[0]
    if last:
        u0, u1, near, acc_in = refs[:4]
        mine_ref, other_ref, parcel, f_s, c_s, wd_ref, acc = refs[4:]
        pairs = [(u0, u1, swapped[0], parcel)]
    else:
        near, sources, refs = refs[0], refs[1:7], refs[7:]
        (acc, pg_ref, parcel_r, parcel_l), refs = refs[:4], refs[4:]
        held, (sems, f_s, c_s, wd_ref) = refs[:6], refs[6:]
        copies = [
            pltpu.make_async_copy(source, place, sems.at[i])
            for i, (source, place) in enumerate(zip(sources, held))
        ]
        for copy in copies:
            copy.start()
        f_ref, c_ref, r0, r1, l0, l1 = held
        acc_in = None
        pairs = [
            (None, None, None, pg_ref),
            (r0, r1, swapped[0], parcel_r),
            (l0, l1, swapped[1], parcel_l),
        ]
    up_at, down_at = core, 1 - core
    wide = w_ref.shape[1] // 2
    wd_ref[...] = w_ref[:, wide:]
    row = lax.broadcasted_iota(jnp.int32, (HEAD, wide), 0)
    f_s[FULL - 16 : FULL, :] = jnp.zeros((16, D), jnp.bfloat16)
    c_s[FULL - 16 : FULL, :] = jnp.zeros((16, D), jnp.bfloat16)
    for g, (u0, u1, spots, out) in enumerate(pairs):
        if not last:
            copies[2 * g].wait()
            copies[2 * g + 1].wait()
        if u0 is None:
            f_s[0:ROWS, :] = f_ref[...]
            c_s[0:ROWS, :] = c_ref[...]
            at = [0, HALF]
        else:
            f_s[0:HEAD, 0:HALF] = u0[:, 0:HALF]
            f_s[HEAD:ROWS, 0:HALF] = u1[:, 0:HALF]
            f_s[0:HEAD, HALF:D] = near[spots[0] : spots[0] + HEAD, :]
            f_s[HEAD:ROWS, HALF:D] = near[spots[1] : spots[1] + TAIL, :]
            c_s[0:HEAD, :] = u0[:, HALF:]
            c_s[HEAD:ROWS, :] = u1[:, HALF:]
            at = [pl.multiple_of(a, HALF) for a in (core * HALF, (1 - core) * HALF)]
        preact = sum(
            jnp.dot(
                f_s[:, i * HALF : (i + 1) * HALF],
                w_ref[pl.ds(at[i], HALF), 0:wide],
                preferred_element_type=jnp.float32,
            )
            for i in range(2)
        )
        cumulative = 0.5 * (1.0 + lax.erf(preact * reciprocal_root))
        density = normal_peak * jnp.exp(-0.5 * preact * preact)
        hidden = (preact * cumulative).astype(jnp.bfloat16)
        back = jnp.dot(c_s[...], wd_ref[...], preferred_element_type=jnp.float32)
        pg = (back * (cumulative + preact * density)).astype(jnp.bfloat16)
        if u0 is None:
            out[...] = pg[:ROWS]
        else:
            out[0:HALF, :] = pack_lanes(w_ref[:, 0:wide], HALF)
            out[HALF:, :] = pack_lanes(pg, HEAD)
        zero = jnp.zeros((), jnp.bfloat16)
        cuts = (slice(0, HEAD), slice(FULL - HEAD, FULL))
        keep = (row < PATCHES, row >= PATCHES - (FULL - HEAD))

        def add(index, at, source, lanes, right):
            each = [dot_rows(source[cut, lanes], right[i]) for i, cut in enumerate(cuts)]
            total = jnp.concatenate(
                [each[0] + each[1], each[0] * each[0] + each[1] * each[1]], axis=1
            )
            span = pl.ds(at, HALF)
            if g == 0 and last:
                acc[index, span, :] = acc_in[index, span, :] + total
            elif g == 0:
                acc[index, span, :] = total
            else:
                acc[index, span, :] = acc[index, span, :] + total

        by_image = [
            [jnp.where(k, v[cut], zero) for cut, k in zip(cuts, keep)] for v in (pg, hidden)
        ]
        for i in range(2):
            lanes = slice(i * HALF, (i + 1) * HALF)
            add(up_at, at[i], f_s, lanes, by_image[0])
            add(down_at, i * HALF, c_s, lanes, by_image[1])
    if last:
        mine_ref[...] = acc[0]
        other_ref[...] = acc[1]


def inside(array):
    return pltpu.with_memory_space_constraint(array, pltpu.VMEM)


def outside(array):
    return pltpu.with_memory_space_constraint(array, pltpu.HBM)


def gathered(parts, place):
    return pl.pallas_call(
        gather_kernel,
        out_shape=pltpu.VMEM((sum(-(-p.shape[0] // 16) * 16 for p in parts), HALF), jnp.bfloat16),
        in_specs=[VMEM] * len(parts),
        out_specs=VMEM,
        compiler_params=pltpu.CompilerParams(vmem_limit_bytes=4 << 20),
    )(*map(place, parts))


def run_groups(core, weights, ins, far_ins, swapped, last):
    wide = weights.shape[1] // 2
    sums = pltpu.VMEM((D, 2 * wide), jnp.float32)
    parcel = pltpu.VMEM((HALF + HEAD, 2 * wide), jnp.bfloat16)
    pair = pltpu.VMEM((FULL, D), jnp.bfloat16)
    scratch = [pltpu.VMEM(a.shape, a.dtype) for a in far_ins]
    if far_ins:
        scratch.append(pltpu.SemaphoreType.DMA((len(far_ins),)))
    scratch += [pair, pair, pltpu.VMEM((D, wide), jnp.bfloat16)]
    if last:
        out_shape = [sums, sums, parcel]
        scratch.append(pltpu.VMEM((2, D, 2 * wide), jnp.float32))
    else:
        out_shape = [
            pltpu.VMEM((2, D, 2 * wide), jnp.float32),
            pltpu.VMEM((ROWS, wide), jnp.bfloat16),
            parcel,
            parcel,
        ]
    groups = 1 if last else 3
    return pl.pallas_call(
        lambda *refs: groups_kernel(*refs, swapped=swapped, last=last),
        out_shape=out_shape,
        in_specs=[SMEM] + [VMEM] * (len(ins) + 1) + [ANY] * len(far_ins),
        out_specs=[VMEM] * len(out_shape),
        scratch_shapes=scratch,
        compiler_params=pltpu.CompilerParams(vmem_limit_bytes=24 << 20),
        cost_estimate=pl.CostEstimate(
            flops=groups * ROWS * D * wide * 8,
            transcendentals=2 * groups * ROWS * wide,
            bytes_accessed=6 << 20,
        ),
    )(core, inside(weights), *map(inside, ins), *map(outside, far_ins))


def input_kernel(at_ref, pg_ref, w_ref, *refs):
    parcels, outs, (up_s, pg_s) = refs[:3], refs[3:-2], refs[-2:]
    wide = pg_ref.shape[1]
    for i, parcel in enumerate(parcels):
        up_s[i, 0:HALF] = parcel[0:HALF, 0:wide]
        up_s[i, HALF:D] = parcel[0:HALF, wide:]
        pg_s[i, 0:HEAD] = parcel[HALF:, 0:wide]
        pg_s[i, FULL - HEAD : FULL] = parcel[HALF:, wide:]
    for k, out in enumerate(outs):
        at = pl.multiple_of(((at_ref[0] + k) % len(outs)) * wide, wide)
        span = pl.ds(at, wide)

        def product(left, right):
            return lax.dot_general(
                left, right, (((1,), (1,)), ((), ())), preferred_element_type=jnp.float32
            )

        value = product(pg_ref[...], w_ref[span, 0:wide])
        for i in range(len(parcels)):
            value = value + product(pg_s[i, 0:ROWS], up_s[i, span, :])
        out[...] = value


def statistics_kernel(
    core_ref, mine_ref, other_ref, pu_ref, pd_ref, ru_ref, rd_ref, nu_ref, nd_ref, sum_ref, *, count
):
    first = core_ref[0] == 0
    blocks, _, width = mine_ref.shape
    wide = width // 2

    def laid(ref):
        tiles = [ref[i] for i in range(blocks)]
        return [
            jnp.concatenate([t[:, cut] for t in tiles], axis=1)
            for cut in (slice(0, wide), slice(wide, width))
        ]

    mine, other = laid(mine_ref), laid(other_ref)
    local = None
    for ours, p_ref, raw_ref, new_ref in ((first, pu_ref, ru_ref, nu_ref), (~first, pd_ref, rd_ref, nd_ref)):
        grad, square = (jnp.where(ours, m, o) for m, o in zip(mine, other))
        new = (1.0 - average_rate) * p_ref[...] + average_rate * (square / (2 * count))
        raw = (grad / 2) / (new + damping)
        new_ref[...] = new
        raw_ref[...] = raw
        part = jnp.sum(raw * raw, axis=0, keepdims=True)
        local = part if local is None else local + part
    folded = sum(local[:, i : i + 128] for i in range(0, local.shape[1], 128))
    sum_ref[...] = jnp.broadcast_to(folded.reshape(1, 1, 128), sum_ref.shape)


def update_kernel(sum_ref, mu_ref, md_ref, ru_ref, rd_ref, nu_ref, nd_ref):
    root_mean = jnp.sqrt(jnp.sum(sum_ref[...], keepdims=True)[0] / (2 * D * FF))
    factor = step_rate * (1.0 / jnp.maximum(clip_level, root_mean))
    nu_ref[...] = mu_ref[...] - factor * ru_ref[...]
    nd_ref[...] = md_ref[...] - factor * rd_ref[...]


def shards(
    features, out_cotangent, mean_up, precision_up, noise_up, mean_down, precision_down, noise_down
):
    core = lax.axis_index("mc").astype(jnp.int32)
    nz, nx, ny = lax.axis_size("z"), lax.axis_size("x"), lax.axis_size("mp")
    rows, cols = mean_up.shape
    wide = cols // nx
    core_at = core.reshape(1)
    cotangent = out_cotangent[0]

    u0, u1, payload = pl.pallas_call(
        prepare_kernel,
        out_shape=[
            pltpu.VMEM((HEAD, HALF + D), jnp.bfloat16),
            pltpu.VMEM((TAIL, HALF + D), jnp.bfloat16),
            pltpu.VMEM((nz, nx, rows, 2 * wide), jnp.bfloat16),
        ],
        in_specs=[SMEM] + [VMEM] * 8,
        out_specs=[VMEM] * 3,
        compiler_params=pltpu.CompilerParams(vmem_limit_bytes=16 << 20),
        name="prepare",
    )(
        core_at,
        *[
            pltpu.with_memory_space_constraint(a, pltpu.HBM)
            for a in (
                features, cotangent, mean_up, precision_up, noise_up[0],
                mean_down, precision_down, noise_down[0],
            )
        ],
    )
    r0 = shift(u0, "x", 1)
    l1 = shift(u1, "x", -1)
    r1 = shift(u1, "x", 1)
    l0 = shift(u0, "x", -1)

    weights = lax.all_to_all(
        payload.reshape(nz * nx, rows, 2 * wide), DP, 0, 0, tiled=True
    ).reshape(D, 2 * wide)

    f0 = shift(r0, "x", 1)
    f1 = shift(l1, "x", -1)
    near = gathered([r0, l0, r1, l1], outside)
    near = shift(near, "mc", 1)
    spots = ((0, 2 * HEAD), (HEAD, HEAD + FULL))
    far = shift(gathered([f0, f1], inside), "mc", 1)

    acc, pg, parcel_r, parcel_l = run_groups(
        core_at, weights, [near], [features, cotangent, r0, r1, l0, l1], spots, False
    )
    parcel_r = shift(parcel_r, "x", -1)
    parcel_l = shift(parcel_l, "x", 1)
    mine, other, parcel_f = run_groups(core_at, weights, [f0, f1, far, acc], [], ((0, HEAD),), True)

    both = mine + shift(other, "mc", 1)
    parcel_f = shift(parcel_f, "x", 2)
    is_grad = lax.broadcasted_iota(jnp.int32, both.shape, 1) < wide
    root = jnp.sqrt(jnp.abs(both)) * jnp.where(is_grad, grad_unit, 1.0 / square_unit)
    packed = jnp.where(both < 0.0, -root, root).astype(jnp.float16)
    got = lax.all_to_all(packed.reshape(nz * nx, rows, 2 * wide), DP, 0, 0, tiled=True)
    got = got.astype(jnp.float32).reshape(nz, nx, rows, 2 * wide)
    is_grad = lax.broadcasted_iota(jnp.int32, got.shape, 3) < wide
    got = jnp.where(
        is_grad, got * jnp.abs(got) / (grad_unit * grad_unit), (square_unit * got) * (square_unit * got)
    )
    total = jnp.sum(got, axis=0)
    traded = shift(total, "mc", 1)

    tile = pltpu.VMEM((ROWS, D // ny), jnp.float32)
    tiles = pl.pallas_call(
        input_kernel,
        out_shape=[tile] * ny,
        in_specs=[SMEM] + [VMEM] * 5,
        out_specs=[VMEM] * ny,
        scratch_shapes=[
            pltpu.VMEM((3, D, wide), jnp.bfloat16),
            pltpu.VMEM((3, FULL, wide), jnp.bfloat16),
        ],
        compiler_params=pltpu.CompilerParams(vmem_limit_bytes=16 << 20),
        cost_estimate=pl.CostEstimate(
            flops=ROWS * D * cols * 2, transcendentals=0, bytes_accessed=4 << 20
        ),
        name="input_grad",
    )(lax.axis_index("mp").astype(jnp.int32).reshape(1), *map(inside, (pg, weights, parcel_r, parcel_l, parcel_f)))
    tiles = [tiles[0]] + [shift(tiles[k], "mp", k) for k in range(1, ny)]
    input_grad = sum(tiles[1:], tiles[0]).astype(jnp.bfloat16)[None]

    group = nz * nx * ny
    whole = jax.ShapeDtypeStruct((rows, cols), jnp.float32)
    kept = pltpu.VMEM((rows, cols), jnp.float32)
    raw_up, raw_down, precision_new_up, precision_new_down, local = pl.pallas_call(
        lambda *refs: statistics_kernel(*refs, count=2 * nz * nx),
        out_shape=[kept, kept, whole, whole, jax.ShapeDtypeStruct((group, 1, 128), jnp.float32)],
        in_specs=[SMEM] + [VMEM] * 4,
        out_specs=[VMEM] * 5,
        compiler_params=pltpu.CompilerParams(vmem_limit_bytes=8 << 20),
        name="statistics",
    )(core.reshape(1), inside(total), inside(traded), inside(precision_up), inside(precision_down))
    everyone = lax.all_to_all(local, ZXY, 0, 0, tiled=True)
    mean_new_up, mean_new_down = pl.pallas_call(
        update_kernel,
        out_shape=[whole, whole],
        in_specs=[VMEM] * 5,
        out_specs=[VMEM] * 2,
        compiler_params=pltpu.CompilerParams(vmem_limit_bytes=8 << 20),
        name="update",
    )(*map(inside, (everyone, mean_up, mean_down, raw_up, raw_down)))
    return (mean_new_up, precision_new_up, mean_new_down, precision_new_down, input_grad)


def solution(mesh):
    split = Mesh(
        mesh.devices.reshape(8, 4, mesh.shape["mp"], mesh.shape["mc"]), ("z", "x", "mp", "mc")
    )
    placed = (
        P(DP, None),
        P("mc", DP, None),
        P(DP, "mp"),
        P(DP, "mp"),
        P("mc", DP, "mp"),
        P(DP, "mp"),
        P(DP, "mp"),
        P("mc", DP, "mp"),
    )

    def step(*args):
        return shards(*args)

    step = jax.shard_map(
        step,
        mesh=split,
        in_specs=placed,
        out_specs=(P(DP, "mp"), P(DP, "mp"), P(DP, "mp"), P(DP, "mp"), P("mc", DP, "mp")),
        check_vma=False,
    )
    return step
```

```python
import jax
import jax.numpy as jnp
from jax import lax
from jax.experimental import pallas as pl
from jax.experimental.pallas import tpu as pltpu
from jax.sharding import Mesh
from jax.sharding import PartitionSpec as P


D = 768
FF = 3072
PATCHES = 197
ROWS = 2 * PATCHES
HEAD = 208
TAIL = ROWS - HEAD
FULL = 400
STEP = 48
QUARTERS = STEP + HEAD - 3 * STEP
HALF = D // 2
DP = ("z", "x")
ZXY = ("z", "x", "mp")

reciprocal_root = 0.7071067811865476
normal_peak = 0.3989422804014327
tempering = 100.0
damping = 4.0
average_rate = 0.25
step_rate = 0.05
clip_level = 0.01
square_unit = 256.0
grad_unit = 8.0

SMEM = pl.BlockSpec(memory_space=pltpu.SMEM)
VMEM = pl.BlockSpec(memory_space=pltpu.VMEM)
ANY = pl.BlockSpec(memory_space=pl.ANY)


def shift(value, axis, k):
    n = lax.axis_size(axis)
    return lax.ppermute(value, axis, [(i, (i + k) % n) for i in range(n)])


def prepare_kernel(
    at_ref, f_ref, c_ref, mu_ref, pu_ref, nu_ref, md_ref, pd_ref, nd_ref,
    head_ref, tail_ref, right_ref, left_ref, w_ref, u_s,
):
    first = at_ref[0] == 0
    u_s[FULL - 16 : FULL] = jnp.zeros((16, HALF + D), jnp.bfloat16)
    u_s[0:ROWS, 0:HALF] = jnp.where(first, f_ref[:, 0:HALF], f_ref[:, HALF:D])
    u_s[0:ROWS, HALF:] = c_ref[...]
    head_ref[...] = u_s[0:HEAD]
    tail_ref[...] = u_s[HEAD:ROWS]
    at = at_ref[1] * STEP
    right_ref[...] = u_s[pl.ds(pl.multiple_of(HEAD + at, 16), STEP)]
    left_ref[...] = u_s[pl.ds(pl.multiple_of(at, 16), HEAD - 3 * STEP)]
    nz, nx, _, width = w_ref.shape

    def drawn(m, p, n):
        spread = 1.0 / jnp.sqrt(tempering * (p[...] + damping))
        return m[...] + spread * n[...]

    up, down = drawn(mu_ref, pu_ref, nu_ref), drawn(md_ref, pd_ref, nd_ref)
    wide = width // 2
    for i in range(nx):
        cut = slice(i * wide, (i + 1) * wide)
        both = jnp.concatenate([up[:, cut], down[:, cut]], axis=1).astype(jnp.bfloat16)
        for k in range(nz):
            w_ref[k, i] = both


def dot_rows(left, right):
    return lax.dot_general(
        left, right, (((0,), (0,)), ((), ())), preferred_element_type=jnp.float32
    )


def join_kernel(right_ref, left_ref, out_ref):
    out_ref[0:STEP] = right_ref[...]
    out_ref[STEP:] = left_ref[...]


def gather_kernel(*refs):
    at = 0
    for ref in refs[:-1]:
        refs[-1][at : at + ref.shape[0], :] = ref[:, 0:HALF]
        at += -(-ref.shape[0] // 16) * 16


def pack_lanes(value, rows):
    return jnp.concatenate([value[:rows], value[value.shape[0] - rows :]], axis=1)


def groups_kernel(at_ref, w_ref, *refs, mode):
    core, mp = at_ref[0], at_ref[1]
    acc_in = None
    if mode == "near":
        near, sources, refs = refs[0], refs[1:9], refs[9:]
        (acc, pg_ref, parcel_r, parcel_l), refs = refs[:4], refs[4:]
    else:
        (near, acc_in, f0, f1), sources, refs = refs[:4], (), refs[4:]
        (mine_ref, other_ref, parcel_f, *refs) = refs
    copies = []
    if sources:
        held, refs = refs[: len(sources)], refs[len(sources) :]
        sems, *refs = refs
        copies = [
            pltpu.make_async_copy(source, place, sems.at[i])
            for i, (source, place) in enumerate(zip(sources, held))
        ]
        for copy in copies:
            copy.start()
    f_s, c_s, wd_ref = refs[:3]
    if mode == "near":
        r0, l1, shared = held[2], held[3], held[4:]
        right, left = [(0, r0, 0, HEAD, 0)], [(HEAD, l1, 0, TAIL, HEAD)]
        for k, part in enumerate(shared):
            turn = (mp + len(shared) - k) % len(shared)
            here = FULL + k * QUARTERS
            right.append((HEAD + turn * STEP, part, 0, STEP, here))
            left.append((turn * STEP, part, STEP, QUARTERS - STEP, here + STEP))
        pairs = [
            ((0, 1), None, pg_ref),
            ((2, 4, 5, 6, 7), right, parcel_r),
            ((3,), left, parcel_l),
        ]
    else:
        acc = refs[3]
        pairs = [((), [(0, f0, 0, HEAD, 0), (HEAD, f1, 0, TAIL, HEAD)], parcel_f)]
    up_at, down_at = core, 1 - core
    wide = w_ref.shape[1] // 2
    wd_ref[...] = w_ref[:, wide:]
    row = lax.broadcasted_iota(jnp.int32, (HEAD, wide), 0)
    f_s[FULL - 16 : FULL, :] = jnp.zeros((16, D), jnp.bfloat16)
    c_s[FULL - 16 : FULL, :] = jnp.zeros((16, D), jnp.bfloat16)
    for g, (needed, pieces, out) in enumerate(pairs):
        for i in needed:
            copies[i].wait()
        if pieces is None:
            f_s[0:ROWS, :] = held[0][...]
            c_s[0:ROWS, :] = held[1][...]
            at = [0, HALF]
        else:
            at = [pl.multiple_of(a, HALF) for a in (core * HALF, (1 - core) * HALF)]
            for start, part, low, size, there in pieces:
                span = pl.ds(start if isinstance(start, int) else pl.multiple_of(start, 16), size)
                f_s[span, 0:HALF] = part[low : low + size, 0:HALF]
                f_s[span, HALF:D] = near[there : there + size, :]
                c_s[span, :] = part[low : low + size, HALF:]
        preact = sum(
            jnp.dot(
                f_s[:, i * HALF : (i + 1) * HALF],
                w_ref[pl.ds(at[i], HALF), 0:wide],
                preferred_element_type=jnp.float32,
            )
            for i in range(2)
        )
        cumulative = 0.5 * (1.0 + lax.erf(preact * reciprocal_root))
        density = normal_peak * jnp.exp(-0.5 * preact * preact)
        hidden = (preact * cumulative).astype(jnp.bfloat16)
        back = jnp.dot(c_s[...], wd_ref[...], preferred_element_type=jnp.float32)
        pg = (back * (cumulative + preact * density)).astype(jnp.bfloat16)
        if pieces is None:
            out[...] = pg[:ROWS]
        else:
            out[0:HALF, :] = pack_lanes(w_ref[:, 0:wide], HALF)
            out[HALF:, :] = pack_lanes(pg, HEAD)
        zero = jnp.zeros((), jnp.bfloat16)
        cuts = (slice(0, HEAD), slice(FULL - HEAD, FULL))
        keep = (row < PATCHES, row >= PATCHES - (FULL - HEAD))

        def add(index, at, source, lanes, right):
            each = [dot_rows(source[cut, lanes], right[i]) for i, cut in enumerate(cuts)]
            total = jnp.concatenate(
                [each[0] + each[1], each[0] * each[0] + each[1] * each[1]], axis=1
            )
            span = pl.ds(at, HALF)
            if g == 0 and acc_in is None:
                acc[index, span, :] = total
            elif g == 0:
                acc[index, span, :] = acc_in[index, span, :] + total
            else:
                acc[index, span, :] = acc[index, span, :] + total

        by_image = [
            [jnp.where(k, v[cut], zero) for cut, k in zip(cuts, keep)] for v in (pg, hidden)
        ]
        for i in range(2):
            lanes = slice(i * HALF, (i + 1) * HALF)
            add(up_at, at[i], f_s, lanes, by_image[0])
            add(down_at, i * HALF, c_s, lanes, by_image[1])
    if mode == "far":
        mine_ref[...] = acc[0]
        other_ref[...] = acc[1]


def inside(array):
    return pltpu.with_memory_space_constraint(array, pltpu.VMEM)


def outside(array):
    return pltpu.with_memory_space_constraint(array, pltpu.HBM)


def gathered(parts, place):
    return pl.pallas_call(
        gather_kernel,
        out_shape=pltpu.VMEM((sum(-(-p.shape[0] // 16) * 16 for p in parts), HALF), jnp.bfloat16),
        in_specs=[VMEM] * len(parts),
        out_specs=VMEM,
        compiler_params=pltpu.CompilerParams(vmem_limit_bytes=4 << 20),
    )(*map(place, parts))


def run_groups(mode, at, weights, ins, far_ins):
    wide = weights.shape[1] // 2
    sums = pltpu.VMEM((D, 2 * wide), jnp.float32)
    every = pltpu.VMEM((2, D, 2 * wide), jnp.float32)
    parcel = pltpu.VMEM((HALF + HEAD, 2 * wide), jnp.bfloat16)
    pair = pltpu.VMEM((FULL, D), jnp.bfloat16)
    scratch = [pltpu.VMEM(a.shape, a.dtype) for a in far_ins]
    if far_ins:
        scratch.append(pltpu.SemaphoreType.DMA((len(far_ins),)))
    scratch += [pair, pair, pltpu.VMEM((D, wide), jnp.bfloat16)]
    if mode == "near":
        out_shape, groups = [every, pltpu.VMEM((ROWS, wide), jnp.bfloat16), parcel, parcel], 3
    else:
        out_shape, groups = [sums, sums, parcel], 1
        scratch.append(pltpu.VMEM((2, D, 2 * wide), jnp.float32))
    return pl.pallas_call(
        lambda *refs: groups_kernel(*refs, mode=mode),
        out_shape=out_shape,
        in_specs=[SMEM] + [VMEM] * (len(ins) + 1) + [ANY] * len(far_ins),
        out_specs=[VMEM] * len(out_shape),
        scratch_shapes=scratch,
        compiler_params=pltpu.CompilerParams(vmem_limit_bytes=24 << 20),
        cost_estimate=pl.CostEstimate(
            flops=groups * ROWS * D * wide * 8,
            transcendentals=2 * groups * ROWS * wide,
            bytes_accessed=6 << 20,
        ),
    )(at, inside(weights), *map(inside, ins), *map(outside, far_ins))


def input_kernel(at_ref, pg_ref, w_ref, *refs):
    parcels, outs, (up_s, pg_s) = refs[:3], refs[3:-2], refs[-2:]
    wide = pg_ref.shape[1]
    for i, parcel in enumerate(parcels):
        up_s[i, 0:HALF] = parcel[0:HALF, 0:wide]
        up_s[i, HALF:D] = parcel[0:HALF, wide:]
        pg_s[i, 0:HEAD] = parcel[HALF:, 0:wide]
        pg_s[i, FULL - HEAD : FULL] = parcel[HALF:, wide:]
    for k, out in enumerate(outs):
        at = pl.multiple_of(((at_ref[0] + k) % len(outs)) * wide, wide)
        span = pl.ds(at, wide)

        def product(left, right):
            return lax.dot_general(
                left, right, (((1,), (1,)), ((), ())), preferred_element_type=jnp.float32
            )

        value = product(pg_ref[...], w_ref[span, 0:wide])
        for i in range(len(parcels)):
            value = value + product(pg_s[i, 0:ROWS], up_s[i, span, :])
        out[...] = value


def statistics_kernel(
    core_ref, mine_ref, other_ref, pu_ref, pd_ref, ru_ref, rd_ref, nu_ref, nd_ref, sum_ref, *, count
):
    first = core_ref[0] == 0
    blocks, _, width = mine_ref.shape
    wide = width // 2

    def laid(ref):
        tiles = [ref[i] for i in range(blocks)]
        return [
            jnp.concatenate([t[:, cut] for t in tiles], axis=1)
            for cut in (slice(0, wide), slice(wide, width))
        ]

    mine, other = laid(mine_ref), laid(other_ref)
    local = None
    for ours, p_ref, raw_ref, new_ref in ((first, pu_ref, ru_ref, nu_ref), (~first, pd_ref, rd_ref, nd_ref)):
        grad, square = (jnp.where(ours, m, o) for m, o in zip(mine, other))
        new = (1.0 - average_rate) * p_ref[...] + average_rate * (square / (2 * count))
        raw = (grad / 2) / (new + damping)
        new_ref[...] = new
        raw_ref[...] = raw
        part = jnp.sum(raw * raw, axis=0, keepdims=True)
        local = part if local is None else local + part
    folded = sum(local[:, i : i + 128] for i in range(0, local.shape[1], 128))
    sum_ref[...] = jnp.broadcast_to(folded.reshape(1, 1, 128), sum_ref.shape)


def update_kernel(sum_ref, mu_ref, md_ref, ru_ref, rd_ref, nu_ref, nd_ref):
    root_mean = jnp.sqrt(jnp.sum(sum_ref[...], keepdims=True)[0] / (2 * D * FF))
    factor = step_rate * (1.0 / jnp.maximum(clip_level, root_mean))
    nu_ref[...] = mu_ref[...] - factor * ru_ref[...]
    nd_ref[...] = md_ref[...] - factor * rd_ref[...]


def shards(
    features, out_cotangent, mean_up, precision_up, noise_up, mean_down, precision_down, noise_down
):
    core = lax.axis_index("mc").astype(jnp.int32)
    nz, nx, ny = lax.axis_size("z"), lax.axis_size("x"), lax.axis_size("mp")
    rows, cols = mean_up.shape
    wide = cols // nx
    mp = lax.axis_index("mp").astype(jnp.int32)
    at = jnp.stack([core, mp])
    cotangent = out_cotangent[0]

    u0, u1, right, left, payload = pl.pallas_call(
        prepare_kernel,
        out_shape=[
            pltpu.VMEM((HEAD, HALF + D), jnp.bfloat16),
            pltpu.VMEM((TAIL, HALF + D), jnp.bfloat16),
            pltpu.VMEM((STEP, HALF + D), jnp.bfloat16),
            pltpu.VMEM((QUARTERS - STEP, HALF + D), jnp.bfloat16),
            pltpu.VMEM((nz, nx, rows, 2 * wide), jnp.bfloat16),
        ],
        in_specs=[SMEM] + [VMEM] * 8,
        out_specs=[VMEM] * 5,
        scratch_shapes=[pltpu.VMEM((FULL, HALF + D), jnp.bfloat16)],
        compiler_params=pltpu.CompilerParams(vmem_limit_bytes=16 << 20),
        name="prepare",
    )(
        at,
        *[
            pltpu.with_memory_space_constraint(a, pltpu.HBM)
            for a in (
                features, cotangent, mean_up, precision_up, noise_up[0],
                mean_down, precision_down, noise_down[0],
            )
        ],
    )
    right = shift(right, "x", 1)
    left = shift(left, "x", -1)
    r0 = shift(u0, "x", 1)
    l1 = shift(u1, "x", -1)

    weights = lax.all_to_all(
        payload.reshape(nz * nx, rows, 2 * wide), DP, 0, 0, tiled=True
    ).reshape(D, 2 * wide)

    joined = pl.pallas_call(
        join_kernel,
        out_shape=pltpu.VMEM((QUARTERS, HALF + D), jnp.bfloat16),
        in_specs=[VMEM] * 2,
        out_specs=VMEM,
        compiler_params=pltpu.CompilerParams(vmem_limit_bytes=4 << 20),
        name="join",
    )(right, left)
    shared = [joined]
    for k in range(1, ny):
        shared.append(shift(joined, "mp", k))
    f0 = shift(r0, "x", 1)
    f1 = shift(l1, "x", -1)
    near = gathered([r0, l1, *shared], outside)
    near = shift(near, "mc", 1)
    far = gathered([f0, f1], inside)
    far = shift(far, "mc", 1)
    acc, pg, parcel_r, parcel_l = run_groups(
        "near", at, weights, [near], [features, cotangent, r0, l1, *shared]
    )
    parcel_r = shift(parcel_r, "x", -1)
    parcel_l = shift(parcel_l, "x", 1)
    mine, other, parcel_f = run_groups("far", at, weights, [far, acc, f0, f1], [])

    both = mine + shift(other, "mc", 1)
    parcel_f = shift(parcel_f, "x", 2)
    is_grad = lax.broadcasted_iota(jnp.int32, both.shape, 1) < wide
    root = jnp.sqrt(jnp.abs(both)) * jnp.where(is_grad, grad_unit, 1.0 / square_unit)
    packed = jnp.where(both < 0.0, -root, root).astype(jnp.float16)
    got = lax.all_to_all(packed.reshape(nz * nx, rows, 2 * wide), DP, 0, 0, tiled=True)
    got = got.astype(jnp.float32).reshape(nz, nx, rows, 2 * wide)
    is_grad = lax.broadcasted_iota(jnp.int32, got.shape, 3) < wide
    got = jnp.where(
        is_grad, got * jnp.abs(got) / (grad_unit * grad_unit), (square_unit * got) * (square_unit * got)
    )
    total = jnp.sum(got, axis=0)
    traded = shift(total, "mc", 1)

    tile = pltpu.VMEM((ROWS, D // ny), jnp.float32)
    tiles = pl.pallas_call(
        input_kernel,
        out_shape=[tile] * ny,
        in_specs=[SMEM] + [VMEM] * 5,
        out_specs=[VMEM] * ny,
        scratch_shapes=[
            pltpu.VMEM((3, D, wide), jnp.bfloat16),
            pltpu.VMEM((3, FULL, wide), jnp.bfloat16),
        ],
        compiler_params=pltpu.CompilerParams(vmem_limit_bytes=16 << 20),
        cost_estimate=pl.CostEstimate(
            flops=ROWS * D * cols * 2, transcendentals=0, bytes_accessed=4 << 20
        ),
        name="input_grad",
    )(mp.reshape(1), *map(inside, (pg, weights, parcel_r, parcel_l, parcel_f)))
    tiles = [tiles[0]] + [shift(tiles[k], "mp", k) for k in range(1, ny)]
    input_grad = sum(tiles[1:], tiles[0]).astype(jnp.bfloat16)[None]

    group = nz * nx * ny
    whole = jax.ShapeDtypeStruct((rows, cols), jnp.float32)
    kept = pltpu.VMEM((rows, cols), jnp.float32)
    raw_up, raw_down, precision_new_up, precision_new_down, local = pl.pallas_call(
        lambda *refs: statistics_kernel(*refs, count=2 * nz * nx),
        out_shape=[kept, kept, whole, whole, jax.ShapeDtypeStruct((group, 1, 128), jnp.float32)],
        in_specs=[SMEM] + [VMEM] * 4,
        out_specs=[VMEM] * 5,
        compiler_params=pltpu.CompilerParams(vmem_limit_bytes=8 << 20),
        name="statistics",
    )(core.reshape(1), inside(total), inside(traded), inside(precision_up), inside(precision_down))
    everyone = lax.all_to_all(local, ZXY, 0, 0, tiled=True)
    mean_new_up, mean_new_down = pl.pallas_call(
        update_kernel,
        out_shape=[whole, whole],
        in_specs=[VMEM] * 5,
        out_specs=[VMEM] * 2,
        compiler_params=pltpu.CompilerParams(vmem_limit_bytes=8 << 20),
        name="update",
    )(*map(inside, (everyone, mean_up, mean_down, raw_up, raw_down)))
    return (mean_new_up, precision_new_up, mean_new_down, precision_new_down, input_grad)


def solution(mesh):
    split = Mesh(
        mesh.devices.reshape(8, 4, mesh.shape["mp"], mesh.shape["mc"]), ("z", "x", "mp", "mc")
    )
    placed = (
        P(DP, None),
        P("mc", DP, None),
        P(DP, "mp"),
        P(DP, "mp"),
        P("mc", DP, "mp"),
        P(DP, "mp"),
        P(DP, "mp"),
        P("mc", DP, "mp"),
    )

    def step(*args):
        return shards(*args)

    step = jax.shard_map(
        step,
        mesh=split,
        in_specs=placed,
        out_specs=(P(DP, "mp"), P(DP, "mp"), P(DP, "mp"), P(DP, "mp"), P("mc", DP, "mp")),
        check_vma=False,
    )
    return step
```

```python
import jax
import jax.numpy as jnp
from jax import lax
from jax.experimental import pallas as pl
from jax.experimental.pallas import tpu as pltpu
from jax.sharding import Mesh
from jax.sharding import PartitionSpec as P


D = 768
FF = 3072
PATCHES = 197
ROWS = 2 * PATCHES
HEAD = 208
TAIL = ROWS - HEAD
FULL = 400
STEP = 48
QUARTERS = STEP + HEAD - 3 * STEP
HALF = D // 2
DP = ("z", "x")
ZXY = ("z", "x", "mp")

reciprocal_root = 0.7071067811865476
normal_peak = 0.3989422804014327
tempering = 100.0
damping = 4.0
average_rate = 0.25
step_rate = 0.05
clip_level = 0.01
square_unit = 256.0
grad_unit = 8.0

SMEM = pl.BlockSpec(memory_space=pltpu.SMEM)
VMEM = pl.BlockSpec(memory_space=pltpu.VMEM)
ANY = pl.BlockSpec(memory_space=pl.ANY)


def shift(value, axis, k):
    n = lax.axis_size(axis)
    return lax.ppermute(value, axis, [(i, (i + k) % n) for i in range(n)])


def prepare_kernel(
    at_ref, f_ref, c_ref, mu_ref, pu_ref, nu_ref, md_ref, pd_ref, nd_ref,
    head_ref, tail_ref, right_ref, left_ref, w_ref, u_s,
):
    first = at_ref[0] == 0
    u_s[FULL - 16 : FULL] = jnp.zeros((16, HALF + D), jnp.bfloat16)
    u_s[0:ROWS, 0:HALF] = jnp.where(first, f_ref[:, 0:HALF], f_ref[:, HALF:D])
    u_s[0:ROWS, HALF:] = c_ref[...]
    head_ref[...] = u_s[0:HEAD]
    tail_ref[...] = u_s[HEAD:ROWS]
    at = at_ref[1] * STEP
    right_ref[...] = u_s[pl.ds(pl.multiple_of(HEAD + at, 16), STEP)]
    left_ref[...] = u_s[pl.ds(pl.multiple_of(at, 16), HEAD - 3 * STEP)]
    nz, nx, _, width = w_ref.shape

    def drawn(m, p, n):
        spread = 1.0 / jnp.sqrt(tempering * (p[...] + damping))
        return m[...] + spread * n[...]

    up, down = drawn(mu_ref, pu_ref, nu_ref), drawn(md_ref, pd_ref, nd_ref)
    wide = width // 2
    for i in range(nx):
        cut = slice(i * wide, (i + 1) * wide)
        both = jnp.concatenate([up[:, cut], down[:, cut]], axis=1).astype(jnp.bfloat16)
        for k in range(nz):
            w_ref[k, i] = both


def dot_rows(left, right):
    return lax.dot_general(
        left, right, (((0,), (0,)), ((), ())), preferred_element_type=jnp.float32
    )


def join_kernel(right_ref, left_ref, out_ref):
    out_ref[0:STEP] = right_ref[...]
    out_ref[STEP:] = left_ref[...]


def gather_kernel(*refs):
    at = 0
    for ref in refs[:-1]:
        refs[-1][at : at + ref.shape[0], :] = ref[:, 0:HALF]
        at += -(-ref.shape[0] // 16) * 16


def pack_lanes(value, rows):
    return jnp.concatenate([value[:rows], value[value.shape[0] - rows :]], axis=1)


def groups_kernel(at_ref, w_ref, *refs, mode):
    core, mp = at_ref[0], at_ref[1]
    acc_in = None
    if mode == "near":
        sources, refs = refs[:9], refs[9:]
        (acc, pg_ref, parcel_r, parcel_l), refs = refs[:4], refs[4:]
    else:
        (near, acc_in, f0, f1), sources, refs = refs[:4], (), refs[4:]
        (mine_ref, other_ref, parcel_f, *refs) = refs
    copies = []
    if sources:
        held, refs = refs[: len(sources)], refs[len(sources) :]
        sems, *refs = refs
        copies = [
            pltpu.make_async_copy(source, place, sems.at[i])
            for i, (source, place) in enumerate(zip(sources, held))
        ]
        for copy in copies:
            copy.start()
    f_s, c_s, wd_ref = refs[:3]
    if mode == "near":
        f_ref, c_ref, near, r0, l1 = held[:5]
        shared = held[5:]
        right, left = [(0, r0, 0, HEAD, 0)], [(HEAD, l1, 0, TAIL, HEAD)]
        for k, part in enumerate(shared):
            turn = (mp + len(shared) - k) % len(shared)
            here = FULL + k * QUARTERS
            right.append((HEAD + turn * STEP, part, 0, STEP, here))
            left.append((turn * STEP, part, STEP, QUARTERS - STEP, here + STEP))
        pairs = [
            ((0, 1), None, pg_ref),
            ((2, 3, 5, 6, 7, 8), right, parcel_r),
            ((4,), left, parcel_l),
        ]
    else:
        acc = refs[3]
        pairs = [((), [(0, f0, 0, HEAD, 0), (HEAD, f1, 0, TAIL, HEAD)], parcel_f)]
    up_at, down_at = core, 1 - core
    wide = w_ref.shape[1] // 2
    wd_ref[...] = w_ref[:, wide:]
    row = lax.broadcasted_iota(jnp.int32, (HEAD, wide), 0)
    f_s[FULL - 16 : FULL, :] = jnp.zeros((16, D), jnp.bfloat16)
    c_s[FULL - 16 : FULL, :] = jnp.zeros((16, D), jnp.bfloat16)
    for g, (needed, pieces, out) in enumerate(pairs):
        for i in needed:
            copies[i].wait()
        if pieces is None:
            f_s[0:ROWS, :] = f_ref[...]
            c_s[0:ROWS, :] = c_ref[...]
            at = [0, HALF]
        else:
            at = [pl.multiple_of(a, HALF) for a in (core * HALF, (1 - core) * HALF)]
            for start, part, low, size, there in pieces:
                span = pl.ds(start if isinstance(start, int) else pl.multiple_of(start, 16), size)
                f_s[span, 0:HALF] = part[low : low + size, 0:HALF]
                f_s[span, HALF:D] = near[there : there + size, :]
                c_s[span, :] = part[low : low + size, HALF:]
        preact = sum(
            jnp.dot(
                f_s[:, i * HALF : (i + 1) * HALF],
                w_ref[pl.ds(at[i], HALF), 0:wide],
                preferred_element_type=jnp.float32,
            )
            for i in range(2)
        )
        cumulative = 0.5 * (1.0 + lax.erf(preact * reciprocal_root))
        density = normal_peak * jnp.exp(-0.5 * preact * preact)
        hidden = (preact * cumulative).astype(jnp.bfloat16)
        back = jnp.dot(c_s[...], wd_ref[...], preferred_element_type=jnp.float32)
        pg = (back * (cumulative + preact * density)).astype(jnp.bfloat16)
        if pieces is None:
            out[...] = pg[:ROWS]
        else:
            out[0:HALF, :] = pack_lanes(w_ref[:, 0:wide], HALF)
            out[HALF:, :] = pack_lanes(pg, HEAD)
        zero = jnp.zeros((), jnp.bfloat16)
        cuts = (slice(0, HEAD), slice(FULL - HEAD, FULL))
        keep = (row < PATCHES, row >= PATCHES - (FULL - HEAD))

        def add(index, at, source, lanes, right):
            each = [dot_rows(source[cut, lanes], right[i]) for i, cut in enumerate(cuts)]
            total = jnp.concatenate(
                [each[0] + each[1], each[0] * each[0] + each[1] * each[1]], axis=1
            )
            span = pl.ds(at, HALF)
            if g == 0 and acc_in is None:
                acc[index, span, :] = total
            elif g == 0:
                acc[index, span, :] = acc_in[index, span, :] + total
            else:
                acc[index, span, :] = acc[index, span, :] + total

        by_image = [
            [jnp.where(k, v[cut], zero) for cut, k in zip(cuts, keep)] for v in (pg, hidden)
        ]
        for i in range(2):
            lanes = slice(i * HALF, (i + 1) * HALF)
            add(up_at, at[i], f_s, lanes, by_image[0])
            add(down_at, i * HALF, c_s, lanes, by_image[1])
    if mode == "far":
        mine_ref[...] = acc[0]
        other_ref[...] = acc[1]


def inside(array):
    return pltpu.with_memory_space_constraint(array, pltpu.VMEM)


def outside(array):
    return pltpu.with_memory_space_constraint(array, pltpu.HBM)


def gathered(parts, places):
    return pl.pallas_call(
        gather_kernel,
        out_shape=pltpu.VMEM((sum(-(-p.shape[0] // 16) * 16 for p in parts), HALF), jnp.bfloat16),
        in_specs=[VMEM] * len(parts),
        out_specs=VMEM,
        compiler_params=pltpu.CompilerParams(vmem_limit_bytes=4 << 20),
    )(*[place(p) for place, p in zip(places, parts)])


def run_groups(mode, at, weights, ins, far_ins):
    wide = weights.shape[1] // 2
    sums = pltpu.VMEM((D, 2 * wide), jnp.float32)
    every = pltpu.VMEM((2, D, 2 * wide), jnp.float32)
    parcel = pltpu.VMEM((HALF + HEAD, 2 * wide), jnp.bfloat16)
    pair = pltpu.VMEM((FULL, D), jnp.bfloat16)
    scratch = [pltpu.VMEM(a.shape, a.dtype) for a in far_ins]
    if far_ins:
        scratch.append(pltpu.SemaphoreType.DMA((len(far_ins),)))
    scratch += [pair, pair, pltpu.VMEM((D, wide), jnp.bfloat16)]
    if mode == "near":
        out_shape, groups = [every, pltpu.VMEM((ROWS, wide), jnp.bfloat16), parcel, parcel], 3
    else:
        out_shape, groups = [sums, sums, parcel], 1
        scratch.append(pltpu.VMEM((2, D, 2 * wide), jnp.float32))
    return pl.pallas_call(
        lambda *refs: groups_kernel(*refs, mode=mode),
        out_shape=out_shape,
        in_specs=[SMEM] + [VMEM] * (len(ins) + 1) + [ANY] * len(far_ins),
        out_specs=[VMEM] * len(out_shape),
        scratch_shapes=scratch,
        compiler_params=pltpu.CompilerParams(vmem_limit_bytes=24 << 20),
        cost_estimate=pl.CostEstimate(
            flops=groups * ROWS * D * wide * 8,
            transcendentals=2 * groups * ROWS * wide,
            bytes_accessed=6 << 20,
        ),
    )(at, inside(weights), *map(inside, ins), *map(outside, far_ins))


def input_kernel(at_ref, pg_ref, w_ref, *refs):
    parcels, outs, (up_s, pg_s) = refs[:3], refs[3:-2], refs[-2:]
    wide = pg_ref.shape[1]
    for i, parcel in enumerate(parcels):
        up_s[i, 0:HALF] = parcel[0:HALF, 0:wide]
        up_s[i, HALF:D] = parcel[0:HALF, wide:]
        pg_s[i, 0:HEAD] = parcel[HALF:, 0:wide]
        pg_s[i, FULL - HEAD : FULL] = parcel[HALF:, wide:]
    for k, out in enumerate(outs):
        at = pl.multiple_of(((at_ref[0] + k) % len(outs)) * wide, wide)
        span = pl.ds(at, wide)

        def product(left, right):
            return lax.dot_general(
                left, right, (((1,), (1,)), ((), ())), preferred_element_type=jnp.float32
            )

        value = product(pg_ref[...], w_ref[span, 0:wide])
        for i in range(len(parcels)):
            value = value + product(pg_s[i, 0:ROWS], up_s[i, span, :])
        out[...] = value


def statistics_kernel(
    core_ref, mine_ref, other_ref, pu_ref, pd_ref, ru_ref, rd_ref, nu_ref, nd_ref, sum_ref, *, count
):
    first = core_ref[0] == 0
    blocks, _, width = mine_ref.shape
    wide = width // 2

    def laid(ref):
        tiles = [ref[i] for i in range(blocks)]
        return [
            jnp.concatenate([t[:, cut] for t in tiles], axis=1)
            for cut in (slice(0, wide), slice(wide, width))
        ]

    mine, other = laid(mine_ref), laid(other_ref)
    local = None
    for ours, p_ref, raw_ref, new_ref in ((first, pu_ref, ru_ref, nu_ref), (~first, pd_ref, rd_ref, nd_ref)):
        grad, square = (jnp.where(ours, m, o) for m, o in zip(mine, other))
        new = (1.0 - average_rate) * p_ref[...] + average_rate * (square / (2 * count))
        raw = (grad / 2) / (new + damping)
        new_ref[...] = new
        raw_ref[...] = raw
        part = jnp.sum(raw * raw, axis=0, keepdims=True)
        local = part if local is None else local + part
    folded = sum(local[:, i : i + 128] for i in range(0, local.shape[1], 128))
    sum_ref[...] = jnp.broadcast_to(folded.reshape(1, 1, 128), sum_ref.shape)


def update_kernel(sum_ref, mu_ref, md_ref, ru_ref, rd_ref, nu_ref, nd_ref):
    root_mean = jnp.sqrt(jnp.sum(sum_ref[...], keepdims=True)[0] / (2 * D * FF))
    factor = step_rate * (1.0 / jnp.maximum(clip_level, root_mean))
    nu_ref[...] = mu_ref[...] - factor * ru_ref[...]
    nd_ref[...] = md_ref[...] - factor * rd_ref[...]


def shards(
    features, out_cotangent, mean_up, precision_up, noise_up, mean_down, precision_down, noise_down
):
    core = lax.axis_index("mc").astype(jnp.int32)
    nz, nx, ny = lax.axis_size("z"), lax.axis_size("x"), lax.axis_size("mp")
    rows, cols = mean_up.shape
    wide = cols // nx
    mp = lax.axis_index("mp").astype(jnp.int32)
    at = jnp.stack([core, mp])
    cotangent = out_cotangent[0]

    u0, u1, right, left, payload = pl.pallas_call(
        prepare_kernel,
        out_shape=[
            pltpu.VMEM((HEAD, HALF + D), jnp.bfloat16),
            pltpu.VMEM((TAIL, HALF + D), jnp.bfloat16),
            pltpu.VMEM((STEP, HALF + D), jnp.bfloat16),
            pltpu.VMEM((QUARTERS - STEP, HALF + D), jnp.bfloat16),
            pltpu.VMEM((nz, nx, rows, 2 * wide), jnp.bfloat16),
        ],
        in_specs=[SMEM] + [VMEM] * 8,
        out_specs=[VMEM] * 5,
        scratch_shapes=[pltpu.VMEM((FULL, HALF + D), jnp.bfloat16)],
        compiler_params=pltpu.CompilerParams(vmem_limit_bytes=16 << 20),
        name="prepare",
    )(
        at,
        *[
            pltpu.with_memory_space_constraint(a, pltpu.HBM)
            for a in (
                features, cotangent, mean_up, precision_up, noise_up[0],
                mean_down, precision_down, noise_down[0],
            )
        ],
    )
    right = shift(right, "x", 1)
    left = shift(left, "x", -1)
    r0 = shift(u0, "x", 1)
    l1 = shift(u1, "x", -1)

    weights = lax.all_to_all(
        payload.reshape(nz * nx, rows, 2 * wide), DP, 0, 0, tiled=True
    ).reshape(D, 2 * wide)

    joined = pl.pallas_call(
        join_kernel,
        out_shape=pltpu.VMEM((QUARTERS, HALF + D), jnp.bfloat16),
        in_specs=[VMEM] * 2,
        out_specs=VMEM,
        compiler_params=pltpu.CompilerParams(vmem_limit_bytes=4 << 20),
        name="join",
    )(right, left)
    shared = [joined]
    for k in range(1, ny):
        shared.append(shift(joined, "mp", k))
    f0 = shift(r0, "x", 1)
    f1 = shift(l1, "x", -1)
    near = gathered([r0, l1, *shared], [outside] * 2 + [inside] * ny)
    near = shift(near, "mc", 1)
    far = gathered([f0, f1], [inside] * 2)
    far = shift(far, "mc", 1)
    acc, pg, parcel_r, parcel_l = run_groups(
        "near", at, weights, [], [features, cotangent, near, r0, l1, *shared]
    )
    parcel_r = shift(parcel_r, "x", -1)
    parcel_l = shift(parcel_l, "x", 1)
    mine, other, parcel_f = run_groups("far", at, weights, [far, acc, f0, f1], [])

    both = mine + shift(other, "mc", 1)
    parcel_f = shift(parcel_f, "x", 2)
    is_grad = lax.broadcasted_iota(jnp.int32, both.shape, 1) < wide
    root = jnp.sqrt(jnp.abs(both)) * jnp.where(is_grad, grad_unit, 1.0 / square_unit)
    packed = jnp.where(both < 0.0, -root, root).astype(jnp.float16)
    got = lax.all_to_all(packed.reshape(nz * nx, rows, 2 * wide), DP, 0, 0, tiled=True)
    got = got.astype(jnp.float32).reshape(nz, nx, rows, 2 * wide)
    is_grad = lax.broadcasted_iota(jnp.int32, got.shape, 3) < wide
    got = jnp.where(
        is_grad, got * jnp.abs(got) / (grad_unit * grad_unit), (square_unit * got) * (square_unit * got)
    )
    total = jnp.sum(got, axis=0)
    traded = shift(total, "mc", 1)

    tile = pltpu.VMEM((ROWS, D // ny), jnp.float32)
    tiles = pl.pallas_call(
        input_kernel,
        out_shape=[tile] * ny,
        in_specs=[SMEM] + [VMEM] * 5,
        out_specs=[VMEM] * ny,
        scratch_shapes=[
            pltpu.VMEM((3, D, wide), jnp.bfloat16),
            pltpu.VMEM((3, FULL, wide), jnp.bfloat16),
        ],
        compiler_params=pltpu.CompilerParams(vmem_limit_bytes=16 << 20),
        cost_estimate=pl.CostEstimate(
            flops=ROWS * D * cols * 2, transcendentals=0, bytes_accessed=4 << 20
        ),
        name="input_grad",
    )(mp.reshape(1), inside(pg), inside(weights), outside(parcel_r), outside(parcel_l), inside(parcel_f))
    tiles = [tiles[0]] + [shift(tiles[k], "mp", k) for k in range(1, ny)]
    input_grad = sum(tiles[1:], tiles[0]).astype(jnp.bfloat16)[None]

    group = nz * nx * ny
    whole = jax.ShapeDtypeStruct((rows, cols), jnp.float32)
    kept = pltpu.VMEM((rows, cols), jnp.float32)
    raw_up, raw_down, precision_new_up, precision_new_down, local = pl.pallas_call(
        lambda *refs: statistics_kernel(*refs, count=2 * nz * nx),
        out_shape=[kept, kept, whole, whole, jax.ShapeDtypeStruct((group, 1, 128), jnp.float32)],
        in_specs=[SMEM] + [VMEM] * 4,
        out_specs=[VMEM] * 5,
        compiler_params=pltpu.CompilerParams(vmem_limit_bytes=8 << 20),
        name="statistics",
    )(core.reshape(1), inside(total), inside(traded), inside(precision_up), inside(precision_down))
    everyone = lax.all_to_all(local, ZXY, 0, 0, tiled=True)
    mean_new_up, mean_new_down = pl.pallas_call(
        update_kernel,
        out_shape=[whole, whole],
        in_specs=[VMEM] * 5,
        out_specs=[VMEM] * 2,
        compiler_params=pltpu.CompilerParams(vmem_limit_bytes=8 << 20),
        name="update",
    )(*map(inside, (everyone, mean_up, mean_down, raw_up, raw_down)))
    return (mean_new_up, precision_new_up, mean_new_down, precision_new_down, input_grad)


def solution(mesh):
    split = Mesh(
        mesh.devices.reshape(8, 4, mesh.shape["mp"], mesh.shape["mc"]), ("z", "x", "mp", "mc")
    )
    placed = (
        P(DP, None),
        P("mc", DP, None),
        P(DP, "mp"),
        P(DP, "mp"),
        P("mc", DP, "mp"),
        P(DP, "mp"),
        P(DP, "mp"),
        P("mc", DP, "mp"),
    )

    def step(*args):
        return shards(*args)

    step = jax.shard_map(
        step,
        mesh=split,
        in_specs=placed,
        out_specs=(P(DP, "mp"), P(DP, "mp"), P(DP, "mp"), P(DP, "mp"), P("mc", DP, "mp")),
        check_vma=False,
    )
    return step
```

```python
import jax
import jax.numpy as jnp
from jax import lax
from jax.experimental import pallas as pl
from jax.experimental.pallas import tpu as pltpu
from jax.sharding import Mesh
from jax.sharding import PartitionSpec as P


D = 768
FF = 3072
PATCHES = 197
ROWS = 2 * PATCHES
HEAD = 208
TAIL = ROWS - HEAD
FULL = 400
STEP = 48
QUARTERS = STEP + HEAD - 3 * STEP
HALF = D // 2
DP = ("z", "x")
ZXY = ("z", "x", "mp")

reciprocal_root = 0.7071067811865476
normal_peak = 0.3989422804014327
tempering = 100.0
damping = 4.0
average_rate = 0.25
step_rate = 0.05
clip_level = 0.01
square_unit = 256.0
grad_unit = 8.0

SMEM = pl.BlockSpec(memory_space=pltpu.SMEM)
VMEM = pl.BlockSpec(memory_space=pltpu.VMEM)
ANY = pl.BlockSpec(memory_space=pl.ANY)


def shift(value, axis, k):
    n = lax.axis_size(axis)
    return lax.ppermute(value, axis, [(i, (i + k) % n) for i in range(n)])


def prepare_kernel(
    at_ref, f_ref, c_ref, head_ref, tail_ref, right_ref, left_ref, u_s
):
    first = at_ref[0] == 0
    u_s[FULL - 16 : FULL] = jnp.zeros((16, HALF + D), jnp.bfloat16)
    u_s[0:ROWS, 0:HALF] = jnp.where(first, f_ref[:, 0:HALF], f_ref[:, HALF:D])
    u_s[0:ROWS, HALF:] = c_ref[...]
    head_ref[...] = u_s[0:HEAD]
    tail_ref[...] = u_s[HEAD:ROWS]
    at = at_ref[1] * STEP
    right_ref[...] = u_s[pl.ds(pl.multiple_of(HEAD + at, 16), STEP)]
    left_ref[...] = u_s[pl.ds(pl.multiple_of(at, 16), HEAD - 3 * STEP)]


def sample_kernel(mu_ref, pu_ref, nu_ref, md_ref, pd_ref, nd_ref, w_ref):
    nz, nx, _, width = w_ref.shape

    def drawn(m, p, n):
        spread = 1.0 / jnp.sqrt(tempering * (p[...] + damping))
        return m[...] + spread * n[...]

    up, down = drawn(mu_ref, pu_ref, nu_ref), drawn(md_ref, pd_ref, nd_ref)
    wide = width // 2
    for i in range(nx):
        cut = slice(i * wide, (i + 1) * wide)
        both = jnp.concatenate([up[:, cut], down[:, cut]], axis=1).astype(jnp.bfloat16)
        for k in range(nz):
            w_ref[k, i] = both


def dot_rows(left, right):
    return lax.dot_general(
        left, right, (((0,), (0,)), ((), ())), preferred_element_type=jnp.float32
    )


def join_kernel(right_ref, left_ref, out_ref):
    out_ref[0:STEP] = right_ref[...]
    out_ref[STEP:] = left_ref[...]


def gather_kernel(*refs):
    at = 0
    for ref in refs[:-1]:
        refs[-1][at : at + ref.shape[0], :] = ref[:, 0:HALF]
        at += -(-ref.shape[0] // 16) * 16


def pack_lanes(value, rows):
    return jnp.concatenate([value[:rows], value[value.shape[0] - rows :]], axis=1)


def groups_kernel(at_ref, w_ref, *refs, mode):
    core, mp = at_ref[0], at_ref[1]
    acc_in = None
    if mode == "near":
        sources, refs = refs[:9], refs[9:]
        (acc, pg_ref, parcel_r, parcel_l), refs = refs[:4], refs[4:]
    else:
        (near, acc_in, f0, f1), sources, refs = refs[:4], (), refs[4:]
        (mine_ref, other_ref, parcel_f, *refs) = refs
    copies = []
    if sources:
        held, refs = refs[: len(sources)], refs[len(sources) :]
        sems, *refs = refs
        copies = [
            pltpu.make_async_copy(source, place, sems.at[i])
            for i, (source, place) in enumerate(zip(sources, held))
        ]
        for copy in copies:
            copy.start()
    f_s, c_s, wd_ref = refs[:3]
    if mode == "near":
        f_ref, c_ref, near, r0, l1 = held[:5]
        shared = held[5:]
        right, left = [(0, r0, 0, HEAD, 0)], [(HEAD, l1, 0, TAIL, HEAD)]
        for k, part in enumerate(shared):
            turn = (mp + len(shared) - k) % len(shared)
            here = FULL + k * QUARTERS
            right.append((HEAD + turn * STEP, part, 0, STEP, here))
            left.append((turn * STEP, part, STEP, QUARTERS - STEP, here + STEP))
        pairs = [
            ((0, 1), None, pg_ref),
            ((2, 3, 5, 6, 7, 8), right, parcel_r),
            ((4,), left, parcel_l),
        ]
    else:
        acc = refs[3]
        pairs = [((), [(0, f0, 0, HEAD, 0), (HEAD, f1, 0, TAIL, HEAD)], parcel_f)]
    up_at, down_at = core, 1 - core
    wide = w_ref.shape[1] // 2
    wd_ref[...] = w_ref[:, wide:]
    row = lax.broadcasted_iota(jnp.int32, (HEAD, wide), 0)
    f_s[FULL - 16 : FULL, :] = jnp.zeros((16, D), jnp.bfloat16)
    c_s[FULL - 16 : FULL, :] = jnp.zeros((16, D), jnp.bfloat16)
    for g, (needed, pieces, out) in enumerate(pairs):
        for i in needed:
            copies[i].wait()
        if pieces is None:
            f_s[0:ROWS, :] = f_ref[...]
            c_s[0:ROWS, :] = c_ref[...]
            at = [0, HALF]
        else:
            at = [pl.multiple_of(a, HALF) for a in (core * HALF, (1 - core) * HALF)]
            for start, part, low, size, there in pieces:
                span = pl.ds(start if isinstance(start, int) else pl.multiple_of(start, 16), size)
                f_s[span, 0:HALF] = part[low : low + size, 0:HALF]
                f_s[span, HALF:D] = near[there : there + size, :]
                c_s[span, :] = part[low : low + size, HALF:]
        preact = sum(
            jnp.dot(
                f_s[:, i * HALF : (i + 1) * HALF],
                w_ref[pl.ds(at[i], HALF), 0:wide],
                preferred_element_type=jnp.float32,
            )
            for i in range(2)
        )
        cumulative = 0.5 * (1.0 + lax.erf(preact * reciprocal_root))
        density = normal_peak * jnp.exp(-0.5 * preact * preact)
        hidden = (preact * cumulative).astype(jnp.bfloat16)
        back = jnp.dot(c_s[...], wd_ref[...], preferred_element_type=jnp.float32)
        pg = (back * (cumulative + preact * density)).astype(jnp.bfloat16)
        if pieces is None:
            out[...] = pg[:ROWS]
        else:
            out[0:HALF, :] = pack_lanes(w_ref[:, 0:wide], HALF)
            out[HALF:, :] = pack_lanes(pg, HEAD)
        zero = jnp.zeros((), jnp.bfloat16)
        cuts = (slice(0, HEAD), slice(FULL - HEAD, FULL))
        keep = (row < PATCHES, row >= PATCHES - (FULL - HEAD))

        def add(index, at, source, lanes, right):
            each = [dot_rows(source[cut, lanes], right[i]) for i, cut in enumerate(cuts)]
            total = jnp.concatenate(
                [each[0] + each[1], each[0] * each[0] + each[1] * each[1]], axis=1
            )
            span = pl.ds(at, HALF)
            if g == 0 and acc_in is None:
                acc[index, span, :] = total
            elif g == 0:
                acc[index, span, :] = acc_in[index, span, :] + total
            else:
                acc[index, span, :] = acc[index, span, :] + total

        by_image = [
            [jnp.where(k, v[cut], zero) for cut, k in zip(cuts, keep)] for v in (pg, hidden)
        ]
        for i in range(2):
            lanes = slice(i * HALF, (i + 1) * HALF)
            add(up_at, at[i], f_s, lanes, by_image[0])
            add(down_at, i * HALF, c_s, lanes, by_image[1])
    if mode == "far":
        mine_ref[...] = acc[0]
        other_ref[...] = acc[1]


def inside(array):
    return pltpu.with_memory_space_constraint(array, pltpu.VMEM)


def outside(array):
    return pltpu.with_memory_space_constraint(array, pltpu.HBM)


def gathered(parts, places):
    return pl.pallas_call(
        gather_kernel,
        out_shape=pltpu.VMEM((sum(-(-p.shape[0] // 16) * 16 for p in parts), HALF), jnp.bfloat16),
        in_specs=[VMEM] * len(parts),
        out_specs=VMEM,
        compiler_params=pltpu.CompilerParams(vmem_limit_bytes=4 << 20),
    )(*[place(p) for place, p in zip(places, parts)])


def run_groups(mode, at, weights, ins, far_ins):
    wide = weights.shape[1] // 2
    sums = pltpu.VMEM((D, 2 * wide), jnp.float32)
    every = pltpu.VMEM((2, D, 2 * wide), jnp.float32)
    parcel = pltpu.VMEM((HALF + HEAD, 2 * wide), jnp.bfloat16)
    pair = pltpu.VMEM((FULL, D), jnp.bfloat16)
    scratch = [pltpu.VMEM(a.shape, a.dtype) for a in far_ins]
    if far_ins:
        scratch.append(pltpu.SemaphoreType.DMA((len(far_ins),)))
    scratch += [pair, pair, pltpu.VMEM((D, wide), jnp.bfloat16)]
    if mode == "near":
        out_shape, groups = [every, pltpu.VMEM((ROWS, wide), jnp.bfloat16), parcel, parcel], 3
    else:
        out_shape, groups = [sums, sums, parcel], 1
        scratch.append(pltpu.VMEM((2, D, 2 * wide), jnp.float32))
    return pl.pallas_call(
        lambda *refs: groups_kernel(*refs, mode=mode),
        out_shape=out_shape,
        in_specs=[SMEM] + [VMEM] * (len(ins) + 1) + [ANY] * len(far_ins),
        out_specs=[VMEM] * len(out_shape),
        scratch_shapes=scratch,
        compiler_params=pltpu.CompilerParams(vmem_limit_bytes=24 << 20),
        cost_estimate=pl.CostEstimate(
            flops=groups * ROWS * D * wide * 8,
            transcendentals=2 * groups * ROWS * wide,
            bytes_accessed=6 << 20,
        ),
    )(at, inside(weights), *map(inside, ins), *map(outside, far_ins))


def input_kernel(at_ref, pg_ref, w_ref, *refs):
    parcels, outs, (up_s, pg_s) = refs[:3], refs[3:-2], refs[-2:]
    wide = pg_ref.shape[1]
    for i, parcel in enumerate(parcels):
        up_s[i, 0:HALF] = parcel[0:HALF, 0:wide]
        up_s[i, HALF:D] = parcel[0:HALF, wide:]
        pg_s[i, 0:HEAD] = parcel[HALF:, 0:wide]
        pg_s[i, FULL - HEAD : FULL] = parcel[HALF:, wide:]
    for k, out in enumerate(outs):
        at = pl.multiple_of(((at_ref[0] + k) % len(outs)) * wide, wide)
        span = pl.ds(at, wide)

        def product(left, right):
            return lax.dot_general(
                left, right, (((1,), (1,)), ((), ())), preferred_element_type=jnp.float32
            )

        value = product(pg_ref[...], w_ref[span, 0:wide])
        for i in range(len(parcels)):
            value = value + product(pg_s[i, 0:ROWS], up_s[i, span, :])
        out[...] = value


def statistics_kernel(
    core_ref, mine_ref, other_ref, pu_ref, pd_ref, ru_ref, rd_ref, nu_ref, nd_ref, sum_ref, *, count
):
    first = core_ref[0] == 0
    blocks, _, width = mine_ref.shape
    wide = width // 2

    def laid(ref):
        tiles = [ref[i] for i in range(blocks)]
        return [
            jnp.concatenate([t[:, cut] for t in tiles], axis=1)
            for cut in (slice(0, wide), slice(wide, width))
        ]

    mine, other = laid(mine_ref), laid(other_ref)
    local = None
    for ours, p_ref, raw_ref, new_ref in ((first, pu_ref, ru_ref, nu_ref), (~first, pd_ref, rd_ref, nd_ref)):
        grad, square = (jnp.where(ours, m, o) for m, o in zip(mine, other))
        new = (1.0 - average_rate) * p_ref[...] + average_rate * (square / (2 * count))
        raw = (grad / 2) / (new + damping)
        new_ref[...] = new
        raw_ref[...] = raw
        part = jnp.sum(raw * raw, axis=0, keepdims=True)
        local = part if local is None else local + part
    folded = sum(local[:, i : i + 128] for i in range(0, local.shape[1], 128))
    sum_ref[...] = jnp.broadcast_to(folded.reshape(1, 1, 128), sum_ref.shape)


def update_kernel(sum_ref, mu_ref, md_ref, ru_ref, rd_ref, nu_ref, nd_ref):
    root_mean = jnp.sqrt(jnp.sum(sum_ref[...], keepdims=True)[0] / (2 * D * FF))
    factor = step_rate * (1.0 / jnp.maximum(clip_level, root_mean))
    nu_ref[...] = mu_ref[...] - factor * ru_ref[...]
    nd_ref[...] = md_ref[...] - factor * rd_ref[...]


def shards(
    features, out_cotangent, mean_up, precision_up, noise_up, mean_down, precision_down, noise_down
):
    core = lax.axis_index("mc").astype(jnp.int32)
    nz, nx, ny = lax.axis_size("z"), lax.axis_size("x"), lax.axis_size("mp")
    rows, cols = mean_up.shape
    wide = cols // nx
    mp = lax.axis_index("mp").astype(jnp.int32)
    at = jnp.stack([core, mp])
    cotangent = out_cotangent[0]

    u0, u1, right, left = pl.pallas_call(
        prepare_kernel,
        out_shape=[
            pltpu.VMEM((HEAD, HALF + D), jnp.bfloat16),
            pltpu.VMEM((TAIL, HALF + D), jnp.bfloat16),
            pltpu.VMEM((STEP, HALF + D), jnp.bfloat16),
            pltpu.VMEM((QUARTERS - STEP, HALF + D), jnp.bfloat16),
        ],
        in_specs=[SMEM] + [VMEM] * 2,
        out_specs=[VMEM] * 4,
        scratch_shapes=[pltpu.VMEM((FULL, HALF + D), jnp.bfloat16)],
        compiler_params=pltpu.CompilerParams(vmem_limit_bytes=16 << 20),
        name="prepare",
    )(at, outside(features), outside(cotangent))
    payload = pl.pallas_call(
        sample_kernel,
        out_shape=pltpu.VMEM((nz, nx, rows, 2 * wide), jnp.bfloat16),
        in_specs=[VMEM] * 6,
        out_specs=VMEM,
        compiler_params=pltpu.CompilerParams(vmem_limit_bytes=16 << 20),
        name="sample",
    )(
        *map(
            outside,
            (mean_up, precision_up, noise_up[0], mean_down, precision_down, noise_down[0]),
        )
    )
    right = shift(right, "x", 1)
    left = shift(left, "x", -1)
    r0 = shift(u0, "x", 1)
    l1 = shift(u1, "x", -1)

    weights = lax.all_to_all(
        payload.reshape(nz * nx, rows, 2 * wide), DP, 0, 0, tiled=True
    ).reshape(D, 2 * wide)

    joined = pl.pallas_call(
        join_kernel,
        out_shape=pltpu.VMEM((QUARTERS, HALF + D), jnp.bfloat16),
        in_specs=[VMEM] * 2,
        out_specs=VMEM,
        compiler_params=pltpu.CompilerParams(vmem_limit_bytes=4 << 20),
        name="join",
    )(right, left)
    shared = [joined]
    for k in range(1, ny):
        shared.append(shift(joined, "mp", k))
    f0 = shift(r0, "x", 1)
    f1 = shift(l1, "x", -1)
    near = gathered([r0, l1, *shared], [outside] * 2 + [inside] * ny)
    near = shift(near, "mc", 1)
    far = gathered([f0, f1], [inside] * 2)
    far = shift(far, "mc", 1)
    acc, pg, parcel_r, parcel_l = run_groups(
        "near", at, weights, [], [features, cotangent, near, r0, l1, *shared]
    )
    parcel_r = shift(parcel_r, "x", -1)
    parcel_l = shift(parcel_l, "x", 1)
    mine, other, parcel_f = run_groups("far", at, weights, [far, acc, f0, f1], [])

    both = mine + shift(other, "mc", 1)
    parcel_f = shift(parcel_f, "x", 2)
    is_grad = lax.broadcasted_iota(jnp.int32, both.shape, 1) < wide
    root = jnp.sqrt(jnp.abs(both)) * jnp.where(is_grad, grad_unit, 1.0 / square_unit)
    packed = jnp.where(both < 0.0, -root, root).astype(jnp.float16)
    got = lax.all_to_all(packed.reshape(nz * nx, rows, 2 * wide), DP, 0, 0, tiled=True)
    got = got.astype(jnp.float32).reshape(nz, nx, rows, 2 * wide)
    is_grad = lax.broadcasted_iota(jnp.int32, got.shape, 3) < wide
    got = jnp.where(
        is_grad, got * jnp.abs(got) / (grad_unit * grad_unit), (square_unit * got) * (square_unit * got)
    )
    total = jnp.sum(got, axis=0)
    traded = shift(total, "mc", 1)

    tile = pltpu.VMEM((ROWS, D // ny), jnp.float32)
    tiles = pl.pallas_call(
        input_kernel,
        out_shape=[tile] * ny,
        in_specs=[SMEM] + [VMEM] * 5,
        out_specs=[VMEM] * ny,
        scratch_shapes=[
            pltpu.VMEM((3, D, wide), jnp.bfloat16),
            pltpu.VMEM((3, FULL, wide), jnp.bfloat16),
        ],
        compiler_params=pltpu.CompilerParams(vmem_limit_bytes=16 << 20),
        cost_estimate=pl.CostEstimate(
            flops=ROWS * D * cols * 2, transcendentals=0, bytes_accessed=4 << 20
        ),
        name="input_grad",
    )(mp.reshape(1), inside(pg), inside(weights), outside(parcel_r), outside(parcel_l), inside(parcel_f))
    tiles = [tiles[0]] + [shift(tiles[k], "mp", k) for k in range(1, ny)]
    input_grad = sum(tiles[1:], tiles[0]).astype(jnp.bfloat16)[None]

    group = nz * nx * ny
    whole = jax.ShapeDtypeStruct((rows, cols), jnp.float32)
    kept = pltpu.VMEM((rows, cols), jnp.float32)
    raw_up, raw_down, precision_new_up, precision_new_down, local = pl.pallas_call(
        lambda *refs: statistics_kernel(*refs, count=2 * nz * nx),
        out_shape=[kept, kept, whole, whole, jax.ShapeDtypeStruct((group, 1, 128), jnp.float32)],
        in_specs=[SMEM] + [VMEM] * 4,
        out_specs=[VMEM] * 5,
        compiler_params=pltpu.CompilerParams(vmem_limit_bytes=8 << 20),
        name="statistics",
    )(core.reshape(1), inside(total), inside(traded), inside(precision_up), inside(precision_down))
    everyone = lax.all_to_all(local, ZXY, 0, 0, tiled=True)
    mean_new_up, mean_new_down = pl.pallas_call(
        update_kernel,
        out_shape=[whole, whole],
        in_specs=[VMEM] * 5,
        out_specs=[VMEM] * 2,
        compiler_params=pltpu.CompilerParams(vmem_limit_bytes=8 << 20),
        name="update",
    )(*map(inside, (everyone, mean_up, mean_down, raw_up, raw_down)))
    return (mean_new_up, precision_new_up, mean_new_down, precision_new_down, input_grad)


def solution(mesh):
    split = Mesh(
        mesh.devices.reshape(8, 4, mesh.shape["mp"], mesh.shape["mc"]), ("z", "x", "mp", "mc")
    )
    placed = (
        P(DP, None),
        P("mc", DP, None),
        P(DP, "mp"),
        P(DP, "mp"),
        P("mc", DP, "mp"),
        P(DP, "mp"),
        P(DP, "mp"),
        P("mc", DP, "mp"),
    )

    def step(*args):
        return shards(*args)

    step = jax.shard_map(
        step,
        mesh=split,
        in_specs=placed,
        out_specs=(P(DP, "mp"), P(DP, "mp"), P(DP, "mp"), P(DP, "mp"), P("mc", DP, "mp")),
        check_vma=False,
    )
    return step
```
